32 devices in a mesh: tm: 2 (over x), gx: 4 (over z), gy: 4 (over y, core).
Axes of the slice: x: 2, y: 2, z: 4, core: 2. Of those that a mesh axis runs over, the one named last changes fastest.
Arguments:
- increment: float32 [2, 137, 64, 512], P('tm', None, 'gx', 'gy'), may hold values from -6 to 6
- dual_state: float32 [2, 137, 64, 512], P('tm', None, 'gx', 'gy'), may hold values from -6 to 6
- forcing: float32 [2, 137, 64, 512], P('tm', None, 'gx', 'gy'), may hold values from -6 to 6
- gradient: float32 [2, 137, 64, 512], P('tm', None, 'gx', 'gy'), may hold values from -3 to 3
- courant_x: float32 [2, 137, 64, 512], P('tm', None, 'gx', 'gy'), may hold values from 0.05 to 0.3
- courant_y: float32 [2, 137, 64, 512], P('tm', None, 'gx', 'gy'), may hold values from 0.05 to 0.3
- error_var: float32 [2, 137, 64, 512], P('tm', None, 'gx', 'gy'), may hold values from 0.2 to 2
- obs_weight: float32 [2, 137, 64, 512], P('tm', None, 'gx', 'gy'), may hold values from 0.2 to 2
- diffusion: float32 [137], replicated, may hold values from 0.02 to 0.1
- level_mix: float32 [137, 137], replicated, may hold values from -0.5 to 0.8
Outputs:
- dual_next: float32 [2, 137, 64, 512], P('tm', None, 'gx', 'gy')
- increment_next: float32 [2, 137, 64, 512], P('tm', None, 'gx', 'gy')
The draws below stay inside these ranges and needn't reach their ends.
All inputs are finite; a program needn't handle non-finite values.
Results may differ from the reference program's by a relative error of at most 0.0001.
Values sent between devices are 32-bit elements; how exact they have to be, the bound alone decides.
A program may use at most 128 MiB of HBM per device.

```python
import math
import jax
import jax.numpy as jnp
from jax import lax

LEVELS = 137
STEPS = 3
SUBWIN = 2
NX = 64
NY = 512


def coherent_field(key):
    level_place = ((jnp.arange(LEVELS, dtype=jnp.float32) + 0.5) / LEVELS)[None, :, None, None]
    along_x = (jnp.arange(NX, dtype=jnp.float32) / NX)[None, None, :, None]
    along_y = (jnp.arange(NY, dtype=jnp.float32) / NY)[None, None, None, :]
    window_place = jnp.arange(SUBWIN, dtype=jnp.float32) / max(SUBWIN - 1, 1)
    window_scale = (0.6 + 0.4 * window_place)[:, None, None, None]
    summed = jnp.zeros((SUBWIN, LEVELS, NX, NY), jnp.float32)
    for mode in range(3):
        mode_key = jax.random.fold_in(key, 31 + mode)
        mode_keys = jax.random.split(mode_key, 6)
        wave_x = jax.random.randint(mode_keys[0], (), 1, 3).astype(jnp.float32)
        wave_y = jax.random.randint(mode_keys[1], (), 1, 3).astype(jnp.float32)
        wave_level = jax.random.randint(mode_keys[2], (), 0, 3).astype(jnp.float32)
        phases = jax.random.uniform(mode_keys[3], (3,), jnp.float32, -math.pi, math.pi)
        strength = jax.random.uniform(mode_keys[4], (), jnp.float32, 0.6, 1.0)
        jitter = 1.0 + 0.1 * jax.random.uniform(mode_keys[5], (SUBWIN, 1, 1, 1), jnp.float32, -1.0, 1.0)
        pattern = jnp.cos(2.0 * math.pi * wave_x * along_x + phases[0])
        pattern = pattern * jnp.cos(2.0 * math.pi * wave_y * along_y + phases[1])
        pattern = pattern * jnp.cos(math.pi * wave_level * level_place + phases[2])
        summed = summed + strength * jitter * pattern
    rough_key = jax.random.fold_in(key, 97)
    smooth = 1.4 * summed
    roughness = 0.5 * jnp.clip(jax.random.normal(rough_key, (SUBWIN, LEVELS, NX, NY), jnp.float32), -2.5, 2.5)
    return window_scale * smooth + roughness


def draw_increment(key, part):
    return coherent_field(jax.random.fold_in(key, 101))


def draw_dual_state(key, part):
    return coherent_field(jax.random.fold_in(key, 202))


def draw_forcing(key, part):
    normal_part = 0.5 * jnp.clip(jax.random.normal(key, (SUBWIN, LEVELS, NX, NY), jnp.float32), -4.0, 4.0)
    growth = 1.0 + 2.0 * jnp.arange(SUBWIN, dtype=jnp.float32) / max(SUBWIN - 1, 1)
    growth = growth[:, None, None, None]
    return normal_part * growth


def draw_level_mix(key, part):
    key_diag = jax.random.fold_in(key, 11)
    key_coupling = jax.random.fold_in(key, 23)
    diagonal = jax.random.uniform(key_diag, (LEVELS,), jnp.float32, 0.5, 0.8)
    coupling = jnp.clip(jax.random.normal(key_coupling, (LEVELS, LEVELS), jnp.float32), -6.0, 6.0) * (0.3 / math.sqrt(LEVELS))
    coupling = coupling * (1.0 - jnp.eye(LEVELS, dtype=jnp.float32))
    return coupling + jnp.diag(diagonal)


def block_levels(key, shape, cuts, least, high):
    loudness, own = 1.0, jax.random.fold_in(key, 6)
    for position, blocks in cuts:
        draws = jnp.exp(jax.random.uniform(jax.random.fold_in(own, position), (blocks,), jnp.float32, least / len(cuts), high / len(cuts)))
        loudness = loudness * jnp.repeat(draws, shape[position] // blocks).reshape([-1 if axis == position else 1 for axis in range(len(shape))])
    return loudness


def bell_draw(stream_key, dims, width, limit, cuts=(), kind=jnp.bfloat16):
    entries = jax.random.normal(stream_key, dims, jnp.float32) * width
    if len(cuts) > 0:
        entries = block_levels(stream_key, dims, cuts, -0.22, 0.18) * entries
    return jnp.clip(entries, min=-limit, max=limit).astype(kind)


def setup_inputs(seed: int = 0) -> dict:
    arg_keys = jax.random.split(jax.random.key(seed), 11)
    increment = draw_increment(jax.random.fold_in(arg_keys[10], 71), 0)
    dual_state = draw_dual_state(jax.random.fold_in(arg_keys[10], 71), 0)
    forcing = draw_forcing(jax.random.fold_in(arg_keys[10], 71), 0)
    gradient = bell_draw(arg_keys[3], (SUBWIN, LEVELS, NX, NY), 0.5, 3.0, ((0, 2), (2, 4), (3, 4)), jnp.float32)
    courant_x = jnp.clip(0.05 + 0.25 * jax.random.uniform(arg_keys[4], (SUBWIN, LEVELS, NX, NY), jnp.float32) ** block_levels(arg_keys[4], (SUBWIN, LEVELS, NX, NY), ((0, 2), (2, 4), (3, 4)), -0.2, 0.2), 0.05, 0.3)
    courant_y = jnp.clip(0.05 + 0.25 * jax.random.uniform(arg_keys[5], (SUBWIN, LEVELS, NX, NY), jnp.float32) ** block_levels(arg_keys[5], (SUBWIN, LEVELS, NX, NY), ((0, 2), (2, 4), (3, 4)), -0.2, 0.2), 0.05, 0.3)
    error_var = jnp.clip(jnp.exp(math.log(2.0) - 2.3025851 * jax.random.uniform(arg_keys[6], (SUBWIN, LEVELS, NX, NY), jnp.float32) ** block_levels(arg_keys[6], (SUBWIN, LEVELS, NX, NY), ((0, 2), (2, 4), (3, 4)), -0.2, 0.2)), 0.2, 2.0)
    obs_weight = jnp.clip(jnp.exp(math.log(2.0) - 2.3025851 * jax.random.uniform(arg_keys[7], (SUBWIN, LEVELS, NX, NY), jnp.float32) ** block_levels(arg_keys[7], (SUBWIN, LEVELS, NX, NY), ((0, 2), (2, 4), (3, 4)), -0.2, 0.2)), 0.2, 2.0)
    diffusion = jnp.clip(jnp.exp(jax.random.uniform(arg_keys[8], (LEVELS,), jnp.float32, math.log(0.02), math.log(0.1))), 0.02, 0.1)
    level_mix = draw_level_mix(jax.random.fold_in(arg_keys[10], 71), 0)
    return dict(increment=increment, dual_state=dual_state, forcing=forcing, gradient=gradient, courant_x=courant_x, courant_y=courant_y, error_var=error_var, obs_weight=obs_weight, diffusion=diffusion, level_mix=level_mix)


def apply_levels(matrix, current):
    return jnp.einsum('lm,mxy->lxy', matrix, current, precision=lax.Precision.HIGHEST)

def neighbours(current):
    padded = jnp.pad(current, ((0, 0), (1, 1), (1, 1)))
    return (padded[:, :-2, 1:-1], padded[:, 2:, 1:-1], padded[:, 1:-1, :-2], padded[:, 1:-1, 2:])

def tangent_step(current, courant_x, courant_y, lower_x, lower_y, spread, level_mix):
    minus_x, plus_x, minus_y, plus_y = neighbours(current)
    advected = (1.0 - courant_x - courant_y - 4.0 * spread) * current + lower_x * minus_x + lower_y * minus_y
    advected = advected + spread * (minus_x + plus_x + minus_y + plus_y)
    return apply_levels(level_mix, advected)

def adjoint_step(current, courant_x, courant_y, spread, level_mix):
    mixed_back = apply_levels(level_mix.T, current)
    minus_x, plus_x, minus_y, plus_y = neighbours(mixed_back)
    result = (1.0 - courant_x - courant_y - 4.0 * spread) * mixed_back + courant_x * plus_x + courant_y * plus_y
    return result + spread * (minus_x + plus_x + minus_y + plus_y)

def reference(increment, dual_state, forcing, gradient, courant_x, courant_y, error_var, obs_weight, diffusion, level_mix):
    spread = diffusion[:, None, None]
    windows = increment.shape[0]
    end_states = []
    back_states = []
    for window in range(windows):
        flow_x = courant_x[window]
        flow_y = courant_y[window]
        lower_x = jnp.pad(flow_x, ((0, 0), (1, 0), (0, 0)))[:, :-1, :]
        lower_y = jnp.pad(flow_y, ((0, 0), (0, 0), (1, 0)))[:, :, :-1]
        forward_state = increment[window]
        for substep in range(STEPS):
            forward_state = tangent_step(forward_state, flow_x, flow_y, lower_x, lower_y, spread, level_mix)
        end_states.append(forward_state)
        if window + 1 < windows:
            adjoint_state = dual_state[window + 1]
        else:
            adjoint_state = jnp.zeros_like(dual_state[0])
        for substep in range(STEPS):
            adjoint_state = adjoint_step(adjoint_state, flow_x, flow_y, spread, level_mix)
        back_states.append(adjoint_state)
    earlier_end = jnp.stack([jnp.zeros_like(increment[0])] + end_states[:-1])
    back_all = jnp.stack(back_states)
    residual_dual = forcing - error_var * dual_state - increment + earlier_end
    residual_incr = gradient - obs_weight * increment - dual_state + back_all
    global_sum = jnp.sum(residual_dual * residual_dual) + jnp.sum(residual_incr * residual_incr)
    cell_count = 2 * residual_dual.size
    root_mean = jnp.sqrt(global_sum / cell_count + 1e-06)
    step_scale = jnp.minimum(1.0, 0.5 / root_mean)
    return (dual_state + step_scale * residual_dual, increment + step_scale * residual_incr)
```

```python
import functools

import jax
import jax.numpy as jnp
from jax import lax
from jax.experimental import pallas as pl
from jax.experimental.pallas import tpu as pltpu
from jax.sharding import PartitionSpec as P

STEPS = 3
MESH = pl.DeviceIdType.MESH
FIELDS = 8


def split(block):
    high = block.astype(jnp.bfloat16)
    return high, (block - high.astype(jnp.float32)).astype(jnp.bfloat16)


def kernel(
    axes,
    increment, dual, forcing, gradient, courant_x, courant_y, error_var, obs_weight, spread_row, matrix,
    out_dual, out_incr, out_scale,
    fwd, adj, ax, by, by_low, inbox, end, end_in, y_low, y_high, y_b, s_low, s_high, s_b,
    dual_v, forcing_v, gradient_v, error_v, obs_v, spread, mat_v, spread_v, mat, mat_t, acc, part, parts,
    load_sem, small_sem, out_sem, u_send, u_recv, e_send, e_recv,
    x_send, x_recv, y_send, y_recv, c_send, c_recv, r_send, r_recv,
):
    windows, nx, ny = axes
    count = windows * nx * ny
    rows, levels, width = dual_v.shape
    pairs = rows // 2
    stack = mat.shape[0] // 2
    k, gx, gy = lax.axis_index("tm"), lax.axis_index("gx"), lax.axis_index("gy")
    me = (k * nx + gx) * ny + gy
    has_next, has_prev = k < windows - 1, k > 0
    x_first, x_last = gx == 0, gx == nx - 1
    y_first, y_last = gy == 0, gy == ny - 1
    lane = lax.broadcasted_iota(jnp.int32, (levels, width), 1)

    def remote(src, dst, send, recv, where):
        return pltpu.make_async_remote_copy(
            src_ref=src, dst_ref=dst, send_sem=send, recv_sem=recv, device_id=where, device_id_type=MESH
        )

    def loop(n, body, start=0):
        def step(i, carry):
            body(i)
            return carry

        lax.fori_loop(start, n, step, 0)

    homes = (
        (increment, lambda i: fwd.at[0, i + 1]),
        (courant_y, lambda i: by.at[i]),
        (courant_x, lambda i: ax.at[i + 1]),
        (dual, lambda i: dual_v.at[i]),
        (forcing, lambda i: forcing_v.at[i]),
        (gradient, lambda i: gradient_v.at[i]),
        (error_var, lambda i: error_v.at[i]),
        (obs_weight, lambda i: obs_v.at[i]),
    )

    def load(f, i):
        source, home = homes[f]
        return pltpu.make_async_copy(source.at[:, i, 0], home(i), load_sem.at[f, i])

    small = (
        pltpu.make_async_copy(spread_row, spread_v, small_sem.at[0]),
        pltpu.make_async_copy(matrix, mat_v, small_sem.at[1]),
    )
    for copy in small:
        copy.start()
    for f in range(FIELDS):
        loop(rows, lambda i, f=f: load(f, i).start())

    barrier = pltpu.get_barrier_semaphore()

    def coords(flat):
        return {"tm": flat // (nx * ny), "gx": (flat // ny) % nx, "gy": flat % ny}

    def greet(d):
        pl.semaphore_signal(barrier, inc=1, device_id=coords((me + d) % count), device_id_type=MESH)

    loop(count, greet, 1)

    for copy in small:
        copy.wait()
    spread[...] = jnp.swapaxes(jnp.broadcast_to(spread_v[...], (width, levels)), 0, 1)
    for source, home in ((mat_v[...], mat), (jnp.swapaxes(mat_v[...], 0, 1), mat_t)):
        high, low = split(source)
        home[0:levels, :] = high
        home[stack : stack + levels, :] = low
    acc[...] = jnp.zeros_like(acc)

    zero = jnp.zeros((levels, width), jnp.float32)

    @pl.when(x_first)
    def _():
        ax[0] = zero
        for s in range(STEPS):
            fwd[s, 0] = zero
            adj[s, 0] = zero

    @pl.when(x_last)
    def _():
        for s in range(STEPS):
            fwd[s, rows + 1] = zero
            adj[s, rows + 1] = zero

    @pl.when(y_first)
    def _():
        y_b[...] = zero
        for s in range(2 * STEPS):
            y_low[s] = zero

    @pl.when(y_last)
    def _():
        for s in range(2 * STEPS):
            y_high[s] = zero

    pl.semaphore_wait(barrier, count - 1)

    def order(t):
        return (t // 2) * (1 - 2 * (t % 2)) + (t % 2) * (pairs - 1)

    def dual_copy(i):
        return remote(dual.at[:, i, 0], inbox.at[i], u_send.at[i], u_recv.at[i], {"tm": k - 1})

    @pl.when(has_prev)
    def _():
        def send(t):
            p = order(t)
            dual_copy(2 * p).start()
            dual_copy(2 * p + 1).start()

        loop(pairs, send)

    def state(n):
        return fwd.at[n] if n < STEPS else adj.at[n - STEPS]

    def x_up(n):
        src = increment.at[:, rows - 1, 0] if n == 0 else state(n).at[rows]
        return remote(src, state(n).at[0], x_send.at[n, 0], x_recv.at[n, 0], {"gx": gx + 1})

    def x_down(n):
        src = increment.at[:, 0, 0] if n == 0 else state(n).at[1]
        return remote(src, state(n).at[rows + 1], x_send.at[n, 1], x_recv.at[n, 1], {"gx": gx - 1})

    def y_up(n):
        return remote(s_high.at[n], y_low.at[n], y_send.at[n, 0], y_recv.at[n, 0], {"gy": gy + 1})

    def y_down(n):
        return remote(s_low.at[n], y_high.at[n], y_send.at[n, 1], y_recv.at[n, 1], {"gy": gy - 1})

    def a_up():
        return remote(courant_x.at[:, rows - 1, 0], ax.at[0], c_send.at[0], c_recv.at[0], {"gx": gx + 1})

    def b_up():
        return remote(s_b, y_b, c_send.at[1], c_recv.at[1], {"gy": gy + 1})

    def start_x(n):
        pl.when(jnp.logical_not(x_last))(lambda: x_up(n).start())
        pl.when(jnp.logical_not(x_first))(lambda: x_down(n).start())

    def start_y(n):
        pl.when(jnp.logical_not(y_last))(lambda: y_up(n).start())
        pl.when(jnp.logical_not(y_first))(lambda: y_down(n).start())

    def wait_halo(n):
        pl.when(jnp.logical_not(x_first))(lambda: x_up(n).wait_recv())
        pl.when(jnp.logical_not(x_last))(lambda: x_down(n).wait_recv())
        pl.when(jnp.logical_not(y_first))(lambda: y_up(n).wait_recv())
        pl.when(jnp.logical_not(y_last))(lambda: y_down(n).wait_recv())

    def sent_halo(n):
        pl.when(jnp.logical_not(x_last))(lambda: x_up(n).wait_send())
        pl.when(jnp.logical_not(x_first))(lambda: x_down(n).wait_send())
        pl.when(jnp.logical_not(y_last))(lambda: y_up(n).wait_send())
        pl.when(jnp.logical_not(y_first))(lambda: y_down(n).wait_send())

    def pack(n, i, value):
        s_high[n] = jnp.where(lane == i, pltpu.roll(value, i + 1, 1), s_high[n])
        s_low[n] = jnp.where(lane == i, pltpu.roll(value, i, 1), s_low[n])

    def around(n, i):
        v = state(n)[i + 1]
        before, after = state(n)[i], state(n)[i + 2]
        left = jnp.where(lane == 0, pltpu.roll(y_low[n], (width - i) % width, 1), pltpu.roll(v, 1, 1))
        right = jnp.where(
            lane == width - 1, pltpu.roll(y_high[n], width - 1 - i, 1), pltpu.roll(v, width - 1, 1)
        )
        return v, before, after, left, right

    def forward_row(n, i):
        v, before, after, left, right = around(n, i)
        s = spread[...]
        flow = (1.0 - 4.0 * s - ax[i + 1] - by[i]) * v + ax[i] * before + by_low[i] * left
        return flow + s * (before + after + left + right)

    def adjoint_row(n, i):
        w, before, after, left, right = around(n, i)
        s = spread[...]
        a, b = ax[i + 1], by[i]
        flow = (1.0 - 4.0 * s - a - b) * w + a * after + b * right
        return flow + s * (before + after + left + right)

    def mixed(mats, first, second):
        high, low = split(jnp.concatenate([first, second], axis=1))
        dot = functools.partial(jnp.dot, preferred_element_type=jnp.float32)
        wide = dot(mats[...], high)
        result = dot(mats[0:levels, :], low) + wide[stack : stack + levels] + wide[0:levels]
        return result[:, :width], result[:, width:]

    def end_copy(i):
        return remote(end.at[i], end_in.at[i], e_send.at[i], e_recv.at[i], {"tm": k + 1})

    def advance(n, row, mats, last):
        def body(t):
            p = order(t)
            for i, value in zip((2 * p, 2 * p + 1), mixed(mats, row(n, 2 * p), row(n, 2 * p + 1))):
                if last:
                    end[i] = value
                else:
                    state(n + 1)[i + 1] = value
                    pack(n + 1, i, value)

        return body

    for f in (0, 1, 2):
        loop(rows, lambda i, f=f: load(f, i).wait())

    @pl.when(has_next)
    def _():
        start_x(0)
        pl.when(jnp.logical_not(x_last))(lambda: a_up().start())

        def pack_inputs(i):
            pack(0, i, fwd[0, i + 1])
            s_b[...] = jnp.where(lane == i, pltpu.roll(by[i], i + 1, 1), s_b[...])

        loop(rows, pack_inputs)
        start_y(0)
        pl.when(jnp.logical_not(y_last))(lambda: b_up().start())
        pl.when(jnp.logical_not(x_first))(lambda: a_up().wait_recv())
        pl.when(jnp.logical_not(y_first))(lambda: b_up().wait_recv())

        def lower(i):
            by_low[i] = jnp.where(
                lane == 0, pltpu.roll(y_b[...], (width - i) % width, 1), pltpu.roll(by[i], 1, 1)
            )

        loop(rows, lower)

        for n in range(STEPS):
            last = n == STEPS - 1
            body = advance(n, forward_row, mat, last)
            wait_halo(n)
            if not last:
                loop(2, body)
                start_x(n + 1)
                loop(pairs, body, 2)
                start_y(n + 1)
            else:
                def send(t):
                    p = order(t)
                    end_copy(2 * p).start()
                    end_copy(2 * p + 1).start()

                def both(t):
                    body(t)
                    pl.when(t > 0)(lambda: send(t - 1))

                loop(pairs, both)
                send(pairs - 1)

        def enter(t):
            p = order(t)
            dual_in = (2 * p, 2 * p + 1)
            for i in dual_in:
                dual_copy(i).wait_recv()
            for i, value in zip(dual_in, mixed(mat_t, inbox[2 * p], inbox[2 * p + 1])):
                adj[0, i + 1] = value
                pack(STEPS, i, value)

        loop(2, enter)
        start_x(STEPS)
        loop(pairs, enter, 2)
        start_y(STEPS)
        for n in range(STEPS, 2 * STEPS - 1):
            body = advance(n, adjoint_row, mat_t, False)
            wait_halo(n)
            loop(2, body)
            start_x(n + 1)
            loop(pairs, body, 2)
            start_y(n + 1)
        wait_halo(2 * STEPS - 1)

    for f in range(3, FIELDS):
        loop(rows, lambda i, f=f: load(f, i).wait())

    def result(ref, out, which, i):
        return pltpu.make_async_copy(ref.at[i], out.at[:, i, 0], out_sem.at[which, i])

    def residual_incr(i, back):
        value = gradient_v[i] - obs_v[i] * fwd[0, i + 1] - dual_v[i]
        if back:
            value = value + adjoint_row(2 * STEPS - 1, i)
        gradient_v[i] = value
        acc[...] += value * value

    def residual_dual(i, earlier):
        value = forcing_v[i] - error_v[i] * dual_v[i] - fwd[0, i + 1]
        if earlier:
            end_copy(i).wait_recv()
            value = value + end_in[i]
        forcing_v[i] = value
        acc[...] += value * value

    def send_out(ref, out, which):
        loop(rows, lambda i: result(ref, out, which, i).start())

    pl.when(has_next)(lambda: loop(rows, lambda i: residual_incr(i, True)))
    pl.when(jnp.logical_not(has_next))(lambda: loop(rows, lambda i: residual_incr(i, False)))
    send_out(gradient_v, out_incr, 1)

    @pl.when(has_prev)
    def _():
        def body(t):
            p = order(t)
            residual_dual(2 * p, True)
            residual_dual(2 * p + 1, True)

        loop(pairs, body)

    pl.when(jnp.logical_not(has_prev))(lambda: loop(rows, lambda i: residual_dual(i, False)))
    send_out(forcing_v, out_dual, 0)

    part[...] = jnp.sum(acc[...], axis=0, keepdims=True)
    parts[me] = part[...]

    def tell(d):
        other = (me + d) % count
        return remote(part, parts.at[me], r_send.at[d], r_recv.at[me], coords(other))

    def hear(d):
        other = (me + count - d) % count
        return remote(part, parts.at[other], r_send.at[d], r_recv.at[other], coords(other))

    loop(count, lambda d: tell(d).start(), 1)
    loop(count, lambda d: hear(d).wait_recv(), 1)
    total = jnp.sum(jnp.sum(parts[...], axis=0), axis=1, keepdims=True)
    cells = 2 * rows * levels * width * count
    root_mean = jnp.sqrt(total / cells + 1e-06)
    out_scale[...] = jnp.broadcast_to(jnp.minimum(1.0, 0.5 / root_mean), out_scale.shape)

    loop(count, lambda d: tell(d).wait_send(), 1)
    for ref, out, which in ((forcing_v, out_dual, 0), (gradient_v, out_incr, 1)):
        loop(rows, lambda i: result(ref, out, which, i).wait())
    pl.when(has_prev)(lambda: loop(rows, lambda i: dual_copy(i).wait_send()))

    @pl.when(has_next)
    def _():
        loop(rows, lambda i: end_copy(i).wait_send())
        pl.when(jnp.logical_not(x_last))(lambda: a_up().wait_send())
        pl.when(jnp.logical_not(y_last))(lambda: b_up().wait_send())
        for n in range(2 * STEPS):
            sent_halo(n)


def local(axes, increment, dual_state, forcing, gradient, courant_x, courant_y, error_var, obs_weight, diffusion, level_mix):
    levels, rows, width = increment.shape[1:]
    count = axes[0] * axes[1] * axes[2]
    stack = -(-levels // 16) * 16
    fields = [
        part.reshape(levels, rows, 1, width)
        for part in (increment, dual_state, forcing, gradient, courant_x, courant_y, error_var, obs_weight)
    ]
    slab = lambda *lead: pltpu.VMEM((*lead, levels, width), jnp.float32)
    dma = lambda *shape: pltpu.SemaphoreType.DMA(shape)
    scratch = [
        slab(STEPS, rows + 2), slab(STEPS, rows + 2), slab(rows + 1), slab(rows), slab(rows),
        slab(rows), slab(rows), slab(rows),
        slab(2 * STEPS), slab(2 * STEPS), slab(), slab(2 * STEPS), slab(2 * STEPS), slab(),
        slab(rows), slab(rows), slab(rows), slab(rows), slab(rows),
        slab(), pltpu.VMEM((levels, levels), jnp.float32), pltpu.VMEM((1, levels), jnp.float32),
        pltpu.VMEM((2 * stack, levels), jnp.bfloat16), pltpu.VMEM((2 * stack, levels), jnp.bfloat16),
        slab(), pltpu.VMEM((1, width), jnp.float32), pltpu.VMEM((count, 1, width), jnp.float32),
        dma(FIELDS, rows), dma(2), dma(2, rows), dma(rows), dma(rows), dma(rows), dma(rows),
        dma(2 * STEPS, 2), dma(2 * STEPS, 2), dma(2 * STEPS, 2), dma(2 * STEPS, 2), dma(2), dma(2),
        dma(count), dma(count),
    ]
    field = jax.ShapeDtypeStruct((levels, rows, 1, width), jnp.float32)
    anywhere = pl.BlockSpec(memory_space=pltpu.HBM)
    residual_dual, residual_incr, scale = pl.pallas_call(
        functools.partial(kernel, axes),
        out_shape=(field, field, jax.ShapeDtypeStruct((1, width), jnp.float32)),
        in_specs=[anywhere] * 10,
        out_specs=(anywhere, anywhere, pl.BlockSpec(memory_space=pltpu.VMEM)),
        scratch_shapes=scratch,
        compiler_params=pltpu.CompilerParams(
            collective_id=0, has_side_effects=True, vmem_limit_bytes=63 * 1024 * 1024
        ),
    )(*fields, diffusion[None, :], level_mix)
    scale = scale[0, 0]
    dual_next = dual_state + scale * residual_dual.reshape(dual_state.shape)
    increment_next = increment + scale * residual_incr.reshape(increment.shape)
    return dual_next, increment_next


def solution(mesh):
    spec = P("tm", None, "gx", "gy")
    axes = tuple(mesh.shape[name] for name in ("tm", "gx", "gy"))
    return jax.shard_map(
        functools.partial(local, axes),
        mesh=mesh,
        in_specs=(spec,) * FIELDS + (P(), P()),
        out_specs=(spec, spec),
        check_vma=False,
    )
```

```python
import functools

import jax
import jax.numpy as jnp
from jax import lax
from jax.experimental import pallas as pl
from jax.experimental.pallas import tpu as pltpu
from jax.sharding import PartitionSpec as P

STEPS = 3
MESH = pl.DeviceIdType.MESH
FIELDS = 8
RIM = STEPS
GROUP = 2 * RIM


def split(block):
    high = block.astype(jnp.bfloat16)
    return high, (block - high.astype(jnp.float32)).astype(jnp.bfloat16)


def kernel(
    axes,
    increment, dual, forcing, gradient, courant_x, courant_y, error_var, obs_weight, spread_row, matrix,
    out_dual, out_incr, out_scale,
    v0, v1, v2, w0, w1, w2, ax, by, by_low, inbox, end, end_in,
    q_own, q_left, q_right, outside, q_dual, out_send, x_msg, x_msg_up, x_msg_down,
    pv, pu, pw, pa, pb,
    dual_v, forcing_v, gradient_v, error_v, obs_v, spread, mat_v, spread_v, mat, mat_t, acc, part, parts,
    load_sem, small_sem, out_sem, u_send, u_recv, e_send, e_recv, o_sem,
    x_send, x_recv, c_send, c_recv, q_send, q_recv, m_send, m_recv, r_send, r_recv, met,
):
    windows, nx, ny = axes
    count = windows * nx * ny
    rows, levels, width = dual_v.shape
    pairs = rows // 2
    quads = pairs // 2
    stack = mat.shape[0] // 2
    k, gx, gy = lax.axis_index("tm"), lax.axis_index("gx"), lax.axis_index("gy")
    me = (k * nx + gx) * ny + gy
    has_next, has_prev = k < windows - 1, k > 0
    not_ = jnp.logical_not
    x_first, x_last = gx == 0, gx == nx - 1
    y_first, y_last = gy == 0, gy == ny - 1
    lane = lax.broadcasted_iota(jnp.int32, (levels, width), 1)
    place = lane // GROUP - 2
    column = lane - (lane // GROUP) * GROUP
    near = column < RIM

    def remote(src, dst, send, recv, where):
        return pltpu.make_async_remote_copy(
            src_ref=src, dst_ref=dst, send_sem=send, recv_sem=recv, device_id=where, device_id_type=MESH
        )

    def loop(n, body, start=0):
        def step(i, carry):
            body(i)
            return carry

        lax.fori_loop(start, n, step, 0)

    homes = (
        (increment, lambda i: v0.at[i + 1]),
        (courant_y, lambda i: by.at[i]),
        (courant_x, lambda i: ax.at[i + 1]),
        (dual, lambda i: dual_v.at[i]),
        (forcing, lambda i: forcing_v.at[i]),
        (gradient, lambda i: gradient_v.at[i]),
        (error_var, lambda i: error_v.at[i]),
        (obs_weight, lambda i: obs_v.at[i]),
    )

    def load(f, i):
        source, home = homes[f]
        return pltpu.make_async_copy(source.at[:, i, 0], home(i), load_sem.at[f, i])

    def loaded(*which):
        for f in which:
            loop(rows, lambda i, f=f: load(f, i).wait())

    barrier = pltpu.get_barrier_semaphore()
    lines = (("tm", k, windows), ("gx", gx, nx), ("gy", gy, ny))

    def greet(semaphore, line):
        name, mine, size = line
        for d in range(1, size):
            other = lax.rem(mine + d, size)
            pl.semaphore_signal(semaphore, inc=1, device_id={name: other}, device_id_type=MESH)

    for line in lines:
        greet(barrier, line)

    small = (
        pltpu.make_async_copy(spread_row, spread_v, small_sem.at[0]),
        pltpu.make_async_copy(matrix, mat_v, small_sem.at[1]),
    )
    for copy in small:
        copy.start()
    for f in range(FIELDS):
        loop(rows, lambda i, f=f: load(f, i).start())

    for copy in small:
        copy.wait()
    spread[...] = jnp.swapaxes(jnp.broadcast_to(spread_v[...], (width, levels)), 0, 1)
    for source, home in ((mat_v[...], mat), (jnp.swapaxes(mat_v[...], 0, 1), mat_t)):
        high, low = split(source)
        home[0:levels, :] = high
        home[stack : stack + levels, :] = low
    acc[...] = jnp.zeros_like(acc)
    zero = jnp.zeros((levels, width), jnp.float32)

    @pl.when(x_first)
    def _():
        ax[0] = zero
        for state in (v0, v1, v2, w0, w1, w2):
            state[0] = zero

    @pl.when(x_last)
    def _():
        for state in (v0, v1, v2, w0, w1, w2):
            state[rows + 1] = zero

    pl.semaphore_wait(barrier, windows + nx + ny - 3)

    def quad_rows(q):
        low, high = quads - 1 - q, quads + q
        return (2 * low, 2 * low + 1, 2 * high, 2 * high + 1)

    def dual_copy(i):
        return remote(dual.at[:, i, 0], inbox.at[i], u_send.at[i], u_recv.at[i], {"tm": k - 1})

    def end_copy(i):
        return remote(end.at[i], end_in.at[i], e_send.at[i], e_recv.at[i], {"tm": k + 1})

    def outside_copy():
        return remote(out_send, outside, o_sem.at[0], o_sem.at[1], {"tm": k - 1})

    def send_quad(copy, q):
        for i in quad_rows(q):
            copy(i).start()

    chain = ((v0, v1, v2), (w0, w1, w2))

    def x_up(c, n):
        state = chain[c][n]
        src = increment.at[:, rows - 1, 0] if (c, n) == (0, 0) else state.at[rows]
        return remote(src, state.at[0], x_send.at[c, n, 0], x_recv.at[c, n, 0], {"gx": gx + 1})

    def x_down(c, n):
        state = chain[c][n]
        src = increment.at[:, 0, 0] if (c, n) == (0, 0) else state.at[1]
        return remote(src, state.at[rows + 1], x_send.at[c, n, 1], x_recv.at[c, n, 1], {"gx": gx - 1})

    def a_up():
        return remote(courant_x.at[:, rows - 1, 0], ax.at[0], c_send, c_recv, {"gx": gx + 1})

    def m_up(n):
        return remote(x_msg.at[n, 0], x_msg_up.at[n], m_send.at[n, 0], m_recv.at[n, 0], {"gx": gx + 1})

    def m_down(n):
        return remote(x_msg.at[n, 1], x_msg_down.at[n], m_send.at[n, 1], m_recv.at[n, 1], {"gx": gx - 1})

    def q_up(n):
        return remote(q_own.at[n], q_left.at[n], q_send.at[n, 0], q_recv.at[n, 0], {"gy": gy + 1})

    def q_down(n):
        return remote(q_own.at[n], q_right.at[n], q_send.at[n, 1], q_recv.at[n, 1], {"gy": gy - 1})

    def start_both(up, down, first, last):
        pl.when(not_(last))(lambda: up.start())
        pl.when(not_(first))(lambda: down.start())

    def heard_both(up, down, first, last):
        pl.when(not_(first))(lambda: up.wait_recv())
        pl.when(not_(last))(lambda: down.wait_recv())

    def sent_both(up, down, first, last):
        pl.when(not_(last))(lambda: up.wait_send())
        pl.when(not_(first))(lambda: down.wait_send())

    def x_start(c, n):
        start_both(x_up(c, n), x_down(c, n), x_first, x_last)

    def x_heard(c, n):
        heard_both(x_up(c, n), x_down(c, n), x_first, x_last)

    def turn(i):
        return GROUP * (i + 2) + RIM

    def pack_into(ref, index, i, value):
        ref[index] = jnp.where(place == i, pltpu.roll(value, turn(i) % width, 1), ref[index])

    inside_x = ((place >= 0) | not_(x_first)) & ((place < rows) | not_(x_last)) & (place < rows + 2)
    own_rows = (place >= 0) & (place < rows)
    inside = (
        inside_x & (not_(near) | not_(y_first)),
        inside_x & (near | not_(y_last)),
    )

    def assemble(target, index, own, left, right):
        target[index, 0] = jnp.where(inside[0] & own_rows, jnp.where(near, left, own), 0.0)
        target[index, 1] = jnp.where(inside[1] & own_rows, jnp.where(near, own, right), 0.0)

    def write_message(n, blocks):
        up, down = zero, zero
        for b, block in enumerate(blocks):
            mine = lane // (2 * GROUP) == b
            up = jnp.where(mine, pltpu.roll(block, (2 * GROUP * b - GROUP * rows) % width, 1), up)
            down = jnp.where(mine, pltpu.roll(block, (2 * GROUP * b - 2 * GROUP) % width, 1), down)
        x_msg[n, 0] = up
        x_msg[n, 1] = down
        start_both(m_up(n), m_down(n), x_first, x_last)

    def read_message(n, refs):
        heard_both(m_up(n), m_down(n), x_first, x_last)
        for b, (ref, index, side) in enumerate(refs):
            low = pltpu.roll(x_msg_up[n], (-2 * GROUP * b) % width, 1)
            high = pltpu.roll(x_msg_down[n], (GROUP * (rows + 2) - 2 * GROUP * b) % width, 1)
            value = jnp.where(place < 0, low, jnp.where(place >= rows, high, ref[index, side]))
            ref[index, side] = jnp.where(inside[side], value, 0.0)

    def mixed(mats, blocks):
        high, low = split(jnp.concatenate(blocks, axis=1))
        dot = functools.partial(jnp.dot, preferred_element_type=jnp.float32)
        wide = dot(mats[...], high)
        result = dot(mats[0:levels, :], low) + wide[stack : stack + levels] + wide[0:levels]
        return [result[:, j * width : (j + 1) * width] for j in range(len(blocks))]

    def sides(block, left_rim, right_rim, i):
        back = (2 * width - turn(i)) % width
        left = pltpu.roll(jnp.where(lane == width - 1, pltpu.roll(left_rim, back, 1), block), 1, 1)
        right = pltpu.roll(jnp.where(lane == 0, pltpu.roll(right_rim, back, 1), block), width - 1, 1)
        return left, right

    def forward_row(state, rim, i):
        v, before, after = state[i + 1], state[i], state[i + 2]
        left, right = sides(v, rim[0], rim[1], i)
        s = spread[...]
        flow = (1.0 - 4.0 * s - ax[i + 1] - by[i]) * v + ax[i] * before + by_low[i] * left
        return flow + s * (before + after + left + right)

    def adjoint_row(state, rim, i):
        w, before, after = state[i + 1], state[i], state[i + 2]
        left, right = sides(w, rim[0], rim[1], i)
        s = spread[...]
        a, b = ax[i + 1], by[i]
        flow = (1.0 - 4.0 * s - a - b) * w + a * after + b * right
        return flow + s * (before + after + left + right)

    def rim_parts(block):
        return (
            pltpu.roll(block, GROUP, 1), pltpu.roll(block, width - GROUP, 1),
            pltpu.roll(block, 1, 1), pltpu.roll(block, width - 1, 1),
        )

    def forward_rim(block, side):
        before, after, left, right = rim_parts(block)
        s, a, b = spread[...], pa[0, side], pb[0, side]
        flow = (1.0 - 4.0 * s - a - b) * block
        flow = flow + pltpu.roll(a, GROUP, 1) * before + pltpu.roll(b, 1, 1) * left
        return jnp.where(inside[side], flow + s * (before + after + left + right), 0.0)

    def adjoint_rim(block, side):
        before, after, left, right = rim_parts(block)
        s, a, b = spread[...], pa[0, side], pb[0, side]
        flow = (1.0 - 4.0 * s - a - b) * block + a * after + b * right
        return jnp.where(inside[side], flow + s * (before + after + left + right), 0.0)

    def advance_rim(ref, n, rule, mats):
        both = mixed(mats, [rule(ref[n, 0], 0), rule(ref[n, 1], 1)])
        ref[n + 1, 0], ref[n + 1, 1] = both

    def forward_quad(n, q):
        which = quad_rows(q)
        values = mixed(mat, [forward_row(chain[0][n], (pv[n, 0], pv[n, 1]), i) for i in which])
        for i, value in zip(which, values):
            if n == STEPS - 1:
                end[i] = value
            else:
                chain[0][n + 1][i + 1] = value

    def adjoint_quad(n, q):
        which = quad_rows(q)
        values = mixed(mat_t, [adjoint_row(chain[1][n], (pw[n, 0], pw[n, 1]), i) for i in which])
        for i, value in zip(which, values):
            chain[1][n + 1][i + 1] = value

    def enter(q):
        which = quad_rows(q)
        for i in which:
            dual_copy(i).wait_recv()
        values = mixed(mat_t, [inbox[i] for i in which])
        for i, value in zip(which, values):
            w0[i + 1] = value
        for i in which:
            pack_into(q_dual, 0, i, inbox[i])

    def enter_rim():
        own, far = q_dual[0], outside[...]
        assemble(pu, 0, own, far, far)

    def result(ref, out, which, i):
        return pltpu.make_async_copy(ref.at[i], out.at[:, i, 0], out_sem.at[which, i])

    def square(value):
        acc[...] += value * value

    def finish_dual(i, earlier):
        value = forcing_v[i]
        if earlier:
            end_copy(i).wait_recv()
            value = value + end_in[i]
            forcing_v[i] = value
        square(value)

    def early_residuals(i):
        d, v = dual_v[i], v0[i + 1]
        forcing_v[i] = forcing_v[i] - error_v[i] * d - v
        gradient_v[i] = gradient_v[i] - obs_v[i] * v - d

    @pl.when(has_prev)
    def _():
        send_quad(dual_copy, quads - 1)
        loaded(3)
        loop(rows, lambda i: pack_into(q_own, 3, i, dual_v[i]))
        start_both(q_up(3), q_down(3), y_first, y_last)
        heard_both(q_up(3), q_down(3), y_first, y_last)
        out_send[...] = jnp.where(near, q_left[3], q_right[3])
        send_quad(dual_copy, quads - 2)
        outside_copy().start()
        loop(quads - 2, lambda t: send_quad(dual_copy, quads - 3 - t))

    @pl.when(has_next)
    def _():
        x_start(0, 0)
        pl.when(not_(x_last))(lambda: a_up().start())
        for n, (f, value) in enumerate(
            ((0, lambda i: v0[i + 1]), (1, lambda i: by[i]), (2, lambda i: ax[i + 1]))
        ):
            loaded(f)
            loop(rows, lambda i, n=n, value=value: pack_into(q_own, n, i, value(i)))
            start_both(q_up(n), q_down(n), y_first, y_last)

    pl.when(not_(has_next))(lambda: loaded(0, 1, 2))
    for line, semaphore in ((lines[1], met.at[0]),):
        greet(semaphore, line)

    @pl.when(has_next)
    def _():
        for n, ref in enumerate((pv, pb, pa)):
            heard_both(q_up(n), q_down(n), y_first, y_last)
            assemble(ref, 0, q_own[n], q_left[n], q_right[n])
        write_message(0, [ref[0, side] for ref in (pv, pb, pa) for side in (0, 1)])

        def lower(i):
            back = (2 * width - turn(i)) % width
            by_low[i] = pltpu.roll(jnp.where(lane == width - 1, pltpu.roll(pb[0, 0], back, 1), by[i]), 1, 1)

        loop(rows, lower)
        loop(quads - 1, lambda q: forward_quad(0, q))
        x_heard(0, 0)
        pl.when(not_(x_first))(lambda: a_up().wait_recv())
        forward_quad(0, quads - 1)
        x_start(0, 1)
        advance_rim(pv, 0, forward_rim, mat)
        loop(quads - 1, lambda q: forward_quad(1, q))
        advance_rim(pv, 1, forward_rim, mat)

        def early_end(q):
            forward_quad(2, q)
            send_quad(end_copy, q)

        loop(quads - 2, early_end)

        read_message(0, [(ref, 0, side) for ref in (pv, pb, pa) for side in (0, 1)])
        advance_rim(pv, 0, forward_rim, mat)
        x_heard(0, 1)
        forward_quad(1, quads - 1)
        x_start(0, 2)
        advance_rim(pv, 1, forward_rim, mat)
        early_end(quads - 2)

    for f in range(3, FIELDS):
        if f == 3:
            pl.when(not_(has_prev))(lambda: loaded(3))
        else:
            loaded(f)
    loop(rows, early_residuals)

    @pl.when(not_(has_prev))
    def _():
        loop(rows, lambda i: finish_dual(i, False))
        loop(rows, lambda i: result(forcing_v, out_dual, 0, i).start())

    pl.semaphore_wait(met.at[0], nx - 1)
    greet(met.at[1], lines[0])

    @pl.when(has_next)
    def _():
        enter(quads - 1)
        x_start(1, 0)
        outside_copy().wait_recv()
        enter_rim()
        write_message(1, [pu[0, 0], pu[0, 1]])
        x_heard(0, 2)
        forward_quad(2, quads - 1)
        send_quad(end_copy, quads - 1)

        def rim_start():
            enter_rim_full()
            pw[0, 0], pw[0, 1] = mixed(mat_t, [pu[0, 0], pu[0, 1]])

        def enter_rim_full():
            own, far = q_dual[0], outside[...]
            for side, (left, right) in enumerate(((far, own), (own, far))):
                value = jnp.where(near, left, right)
                low = pltpu.roll(x_msg_up[1], (-2 * GROUP * side) % width, 1)
                high = pltpu.roll(x_msg_down[1], (GROUP * (rows + 2) - 2 * GROUP * side) % width, 1)
                value = jnp.where(place < 0, low, jnp.where(place >= rows, high, value))
                pu[0, side] = jnp.where(inside[side], value, 0.0)

        loop(quads - 1, lambda t: enter(quads - 2 - t))
        heard_both(m_up(1), m_down(1), x_first, x_last)
        rim_start()
        x_heard(1, 0)
        adjoint_quad(0, quads - 1)
        x_start(1, 1)
        loop(quads - 1, lambda t: adjoint_quad(0, t))
        advance_rim(pw, 0, adjoint_rim, mat_t)
        loop(quads - 1, lambda t: adjoint_quad(1, t))
        x_heard(1, 1)
        adjoint_quad(1, quads - 1)
        x_start(1, 2)
        advance_rim(pw, 1, adjoint_rim, mat_t)

        def finish_incr(q):
            for i in quad_rows(q):
                value = gradient_v[i] + adjoint_row(w2, (pw[2, 0], pw[2, 1]), i)
                gradient_v[i] = value
                square(value)

        loop(quads - 1, finish_incr)
        x_heard(1, 2)
        finish_incr(quads - 1)

    pl.when(not_(has_next))(lambda: loop(rows, lambda i: square(gradient_v[i])))
    loop(rows, lambda i: result(gradient_v, out_incr, 1, i).start())

    @pl.when(has_prev)
    def _():
        def body(q):
            for i in quad_rows(q):
                finish_dual(i, True)
            for i in quad_rows(q):
                result(forcing_v, out_dual, 0, i).start()

        loop(quads, body)

    pl.semaphore_wait(met.at[1], windows - 1)
    part[...] = jnp.sum(acc[...], axis=0, keepdims=True)
    parts[me] = part[...]

    def coords(flat):
        return {"tm": flat // (nx * ny), "gx": (flat // ny) % nx, "gy": flat % ny}

    def tell(d):
        other = (me + d) % count
        return remote(part, parts.at[me], r_send.at[d], r_recv.at[me], coords(other))

    def hear(d):
        other = (me + count - d) % count
        return remote(part, parts.at[other], r_send.at[d], r_recv.at[other], coords(other))

    loop(count, lambda d: tell(d).start(), 1)

    pl.when(has_prev)(lambda: loop(rows, lambda i: dual_copy(i).wait_send()))

    @pl.when(has_prev)
    def _():
        outside_copy().wait_send()
        sent_both(q_up(3), q_down(3), y_first, y_last)

    @pl.when(has_next)
    def _():
        loop(rows, lambda i: end_copy(i).wait_send())
        pl.when(not_(x_last))(lambda: a_up().wait_send())
        for n in range(STEPS):
            sent_both(x_up(0, n), x_down(0, n), x_first, x_last)
            sent_both(x_up(1, n), x_down(1, n), x_first, x_last)
            sent_both(q_up(n), q_down(n), y_first, y_last)
        for n in range(2):
            sent_both(m_up(n), m_down(n), x_first, x_last)

    for ref, out, which in ((forcing_v, out_dual, 0), (gradient_v, out_incr, 1)):
        loop(rows, lambda i: result(ref, out, which, i).wait())
    loop(count, lambda d: hear(d).wait_recv(), 1)
    total = jnp.sum(jnp.sum(parts[...], axis=0), axis=1, keepdims=True)
    cells = 2 * rows * levels * width * count
    root_mean = jnp.sqrt(total / cells + 1e-06)
    out_scale[...] = jnp.broadcast_to(jnp.minimum(1.0, 0.5 / root_mean), out_scale.shape)
    loop(count, lambda d: tell(d).wait_send(), 1)


def update(scale, dual, increment, residual_dual, residual_incr, dual_next, increment_next):
    dual_next[...] = dual[...] + scale[...] * residual_dual[...]
    increment_next[...] = increment[...] + scale[...] * residual_incr[...]


def local(axes, increment, dual_state, forcing, gradient, courant_x, courant_y, error_var, obs_weight, diffusion, level_mix):
    levels, rows, width = increment.shape[1:]
    count = axes[0] * axes[1] * axes[2]
    stack = -(-levels // 16) * 16
    assert rows % 4 == 0 and GROUP * (rows + 4) <= width
    fields = [
        part.reshape(levels, rows, 1, width)
        for part in (increment, dual_state, forcing, gradient, courant_x, courant_y, error_var, obs_weight)
    ]
    slab = lambda *lead: pltpu.VMEM((*lead, levels, width), jnp.float32)
    dma = lambda *shape: pltpu.SemaphoreType.DMA(shape)
    one = pltpu.SemaphoreType.DMA
    scratch = [
        *[slab(rows + 2)] * 6, slab(rows + 1), slab(rows), slab(rows), slab(rows), slab(rows), slab(rows),
        slab(4), slab(4), slab(4), slab(), slab(1), slab(), slab(2, 2), slab(2), slab(2),
        slab(3, 2), slab(1, 2), slab(3, 2), slab(1, 2), slab(1, 2),
        slab(rows), slab(rows), slab(rows), slab(rows), slab(rows),
        slab(), pltpu.VMEM((levels, levels), jnp.float32), pltpu.VMEM((1, levels), jnp.float32),
        pltpu.VMEM((2 * stack, levels), jnp.bfloat16), pltpu.VMEM((2 * stack, levels), jnp.bfloat16),
        slab(), pltpu.VMEM((1, width), jnp.float32), pltpu.VMEM((count, 1, width), jnp.float32),
        dma(FIELDS, rows), dma(2), dma(2, rows), dma(rows), dma(rows), dma(rows), dma(rows), dma(2),
        dma(2, STEPS, 2), dma(2, STEPS, 2), one, one, dma(4, 2), dma(4, 2), dma(2, 2), dma(2, 2),
        dma(count), dma(count), pltpu.SemaphoreType.REGULAR((2,)),
    ]
    field = jax.ShapeDtypeStruct((levels, rows, 1, width), jnp.float32)
    anywhere = pl.BlockSpec(memory_space=pltpu.HBM)
    residual_dual, residual_incr, scale = pl.pallas_call(
        functools.partial(kernel, axes),
        out_shape=(field, field, jax.ShapeDtypeStruct((1, width), jnp.float32)),
        in_specs=[anywhere] * 10,
        out_specs=(anywhere, anywhere, pl.BlockSpec(memory_space=pltpu.VMEM)),
        scratch_shapes=scratch,
        compiler_params=pltpu.CompilerParams(
            collective_id=0, has_side_effects=True, vmem_limit_bytes=63 * 1024 * 1024
        ),
    )(*fields, diffusion[None, :], level_mix)
    flat = lambda part: part.reshape(levels, rows, width)
    chunk = -(-levels // 4)
    block = pl.BlockSpec((chunk, rows, width), lambda i: (i, 0, 0))
    whole = jax.ShapeDtypeStruct((levels, rows, width), jnp.float32)
    results = pl.pallas_call(
        update,
        grid=(4,),
        out_shape=(whole, whole),
        in_specs=[pl.BlockSpec((1, 1, width), lambda i: (0, 0, 0))] + [block] * 4,
        out_specs=(block, block),
    )(scale.reshape(1, 1, width), *map(flat, (dual_state, increment, residual_dual, residual_incr)))
    return tuple(part.reshape(increment.shape) for part in results)


def solution(mesh):
    spec = P("tm", None, "gx", "gy")
    axes = tuple(mesh.shape[name] for name in ("tm", "gx", "gy"))
    return jax.shard_map(
        functools.partial(local, axes),
        mesh=mesh,
        in_specs=(spec,) * FIELDS + (P(), P()),
        out_specs=(spec, spec),
        check_vma=False,
    )
```

```python
import functools

import jax
import jax.numpy as jnp
from jax import lax
from jax.experimental import pallas as pl
from jax.experimental.pallas import tpu as pltpu
from jax.sharding import PartitionSpec as P

STEPS = 3
MESH = pl.DeviceIdType.MESH
FIELDS = 8
RIM = STEPS
GROUP = 2 * RIM


def split(block):
    high = block.astype(jnp.bfloat16)
    return high, (block - high.astype(jnp.float32)).astype(jnp.bfloat16)


def kernel(
    axes,
    increment, dual, forcing, gradient, courant_x, courant_y, error_var, obs_weight, spread_row, matrix,
    out_dual, out_incr, out_scale,
    v0, v1, v2, w0, w1, w2, ax, by, by_low, inbox, end, end_in,
    q_own, q_left, q_right, outside, q_dual, out_send, x_msg, x_msg_up, x_msg_down,
    pv, pu, pw, pa, pb,
    dual_v, forcing_v, gradient_v, error_v, obs_v, spread, mat_v, spread_v, mat, mat_t, acc, part, parts,
    load_sem, small_sem, u_send, u_recv, e_send, e_recv, o_sem,
    x_send, x_recv, c_send, c_recv, q_send, q_recv, m_send, m_recv, r_send, r_recv, met,
):
    windows, nx, ny = axes
    count = windows * nx * ny
    rows, levels, width = dual_v.shape
    pairs = rows // 2
    quads = pairs // 2
    stack = mat.shape[0] // 2
    k, gx, gy = lax.axis_index("tm"), lax.axis_index("gx"), lax.axis_index("gy")
    me = (k * nx + gx) * ny + gy
    has_next, has_prev = k < windows - 1, k > 0
    not_ = jnp.logical_not
    x_first, x_last = gx == 0, gx == nx - 1
    y_first, y_last = gy == 0, gy == ny - 1
    lane = lax.broadcasted_iota(jnp.int32, (levels, width), 1)
    place = lane // GROUP - 2
    column = lane - (lane // GROUP) * GROUP
    near = column < RIM

    def remote(src, dst, send, recv, where):
        return pltpu.make_async_remote_copy(
            src_ref=src, dst_ref=dst, send_sem=send, recv_sem=recv, device_id=where, device_id_type=MESH
        )

    def loop(n, body, start=0):
        def step(i, carry):
            body(i)
            return carry

        lax.fori_loop(start, n, step, 0)

    homes = (
        (increment, lambda i: v0.at[i + 1]),
        (courant_y, lambda i: by.at[i]),
        (courant_x, lambda i: ax.at[i + 1]),
        (dual, lambda i: dual_v.at[i]),
        (forcing, lambda i: forcing_v.at[i]),
        (gradient, lambda i: gradient_v.at[i]),
        (error_var, lambda i: error_v.at[i]),
        (obs_weight, lambda i: obs_v.at[i]),
    )

    def load(f, i):
        source, home = homes[f]
        return pltpu.make_async_copy(source.at[:, i, 0], home(i), load_sem.at[f])

    def loaded(*which):
        for f in which:
            pltpu.make_async_copy(homes[f][0], homes[f][0], load_sem.at[f]).wait()

    barrier = pltpu.get_barrier_semaphore()
    lines = (("tm", k, windows), ("gx", gx, nx), ("gy", gy, ny))

    def greet(semaphore, line):
        name, mine, size = line
        for d in range(1, size):
            other = lax.rem(mine + d, size)
            pl.semaphore_signal(semaphore, inc=1, device_id={name: other}, device_id_type=MESH)

    for line in lines:
        greet(barrier, line)

    small = (
        pltpu.make_async_copy(spread_row, spread_v, small_sem.at[0]),
        pltpu.make_async_copy(matrix, mat_v, small_sem.at[1]),
    )
    for copy in small:
        copy.start()
    for f in range(FIELDS):
        loop(rows, lambda i, f=f: load(f, i).start())

    for copy in small:
        copy.wait()
    spread[...] = jnp.swapaxes(jnp.broadcast_to(spread_v[...], (width, levels)), 0, 1)
    for source, home in ((mat_v[...], mat), (jnp.swapaxes(mat_v[...], 0, 1), mat_t)):
        high, low = split(source)
        home[0:levels, :] = high
        home[stack : stack + levels, :] = low
    acc[...] = jnp.zeros_like(acc)
    zero = jnp.zeros((levels, width), jnp.float32)

    @pl.when(x_first)
    def _():
        ax[0] = zero
        for state in (v0, v1, v2, w0, w1, w2):
            state[0] = zero

    @pl.when(x_last)
    def _():
        for state in (v0, v1, v2, w0, w1, w2):
            state[rows + 1] = zero

    pl.semaphore_wait(barrier, windows + nx + ny - 3)

    def quad_rows(q):
        low, high = quads - 1 - q, quads + q
        return (2 * low, 2 * low + 1, 2 * high, 2 * high + 1)

    def arrived(semaphores, q):
        whole = dual.at[:, pl.ds(0, 4)]
        remote(whole, whole, u_send, semaphores.at[q], {"tm": k}).wait_recv()

    def left_all(semaphore):
        remote(dual, dual, semaphore, u_recv.at[0], {"tm": k}).wait_send()

    def dual_copy(i, q):
        return remote(dual.at[:, i, 0], inbox.at[i], u_send, u_recv.at[q], {"tm": k - 1})

    def end_copy(i, q):
        return remote(end.at[i], end_in.at[i], e_send, e_recv.at[q], {"tm": k + 1})

    def outside_copy():
        return remote(out_send, outside, o_sem.at[0], o_sem.at[1], {"tm": k - 1})

    def send_quad(copy, q):
        for i in quad_rows(q):
            copy(i, q).start()

    chain = ((v0, v1, v2), (w0, w1, w2))

    def x_up(c, n):
        state = chain[c][n]
        src = increment.at[:, rows - 1, 0] if (c, n) == (0, 0) else state.at[rows]
        return remote(src, state.at[0], x_send.at[c, n, 0], x_recv.at[c, n, 0], {"gx": gx + 1})

    def x_down(c, n):
        state = chain[c][n]
        src = increment.at[:, 0, 0] if (c, n) == (0, 0) else state.at[1]
        return remote(src, state.at[rows + 1], x_send.at[c, n, 1], x_recv.at[c, n, 1], {"gx": gx - 1})

    def a_up():
        return remote(courant_x.at[:, rows - 1, 0], ax.at[0], c_send, c_recv, {"gx": gx + 1})

    def m_up(n):
        return remote(x_msg.at[n, 0], x_msg_up.at[n], m_send.at[n, 0], m_recv.at[n, 0], {"gx": gx + 1})

    def m_down(n):
        return remote(x_msg.at[n, 1], x_msg_down.at[n], m_send.at[n, 1], m_recv.at[n, 1], {"gx": gx - 1})

    def q_up(n):
        return remote(q_own.at[n], q_left.at[n], q_send.at[n, 0], q_recv.at[n, 0], {"gy": gy + 1})

    def q_down(n):
        return remote(q_own.at[n], q_right.at[n], q_send.at[n, 1], q_recv.at[n, 1], {"gy": gy - 1})

    def start_both(up, down, first, last):
        pl.when(not_(last))(lambda: up.start())
        pl.when(not_(first))(lambda: down.start())

    def heard_both(up, down, first, last):
        pl.when(not_(first))(lambda: up.wait_recv())
        pl.when(not_(last))(lambda: down.wait_recv())

    def sent_both(up, down, first, last):
        pl.when(not_(last))(lambda: up.wait_send())
        pl.when(not_(first))(lambda: down.wait_send())

    def x_start(c, n):
        start_both(x_up(c, n), x_down(c, n), x_first, x_last)

    def x_heard(c, n):
        heard_both(x_up(c, n), x_down(c, n), x_first, x_last)

    def turn(i):
        return GROUP * (i + 2) + RIM

    def pack_into(ref, index, which, value):
        packed = ref[index]
        for i in which:
            packed = jnp.where(place == i, pltpu.roll(value(i), turn(i) % width, 1), packed)
        ref[index] = packed

    inside_x = ((place >= 0) | not_(x_first)) & ((place < rows) | not_(x_last)) & (place < rows + 2)
    own_rows = (place >= 0) & (place < rows)
    inside = (
        inside_x & (not_(near) | not_(y_first)),
        inside_x & (near | not_(y_last)),
    )

    def assemble(target, index, own, left, right):
        target[index, 0] = jnp.where(inside[0] & own_rows, jnp.where(near, left, own), 0.0)
        target[index, 1] = jnp.where(inside[1] & own_rows, jnp.where(near, own, right), 0.0)

    def write_message(n, blocks):
        up, down = zero, zero
        for b, block in enumerate(blocks):
            mine = lane // (2 * GROUP) == b
            up = jnp.where(mine, pltpu.roll(block, (2 * GROUP * b - GROUP * rows) % width, 1), up)
            down = jnp.where(mine, pltpu.roll(block, (2 * GROUP * b - 2 * GROUP) % width, 1), down)
        x_msg[n, 0] = up
        x_msg[n, 1] = down
        start_both(m_up(n), m_down(n), x_first, x_last)

    def read_message(n, refs):
        heard_both(m_up(n), m_down(n), x_first, x_last)
        for b, (ref, index, side) in enumerate(refs):
            low = pltpu.roll(x_msg_up[n], (-2 * GROUP * b) % width, 1)
            high = pltpu.roll(x_msg_down[n], (GROUP * (rows + 2) - 2 * GROUP * b) % width, 1)
            value = jnp.where(place < 0, low, jnp.where(place >= rows, high, ref[index, side]))
            ref[index, side] = jnp.where(inside[side], value, 0.0)

    def mixed(mats, blocks):
        high, low = split(jnp.concatenate(blocks, axis=1))
        dot = functools.partial(jnp.dot, preferred_element_type=jnp.float32)
        wide = dot(mats[...], high)
        result = dot(mats[0:levels, :], low) + wide[stack : stack + levels] + wide[0:levels]
        return [result[:, j * width : (j + 1) * width] for j in range(len(blocks))]

    def sides(block, left_rim, right_rim, i):
        back = (2 * width - turn(i)) % width
        left = pltpu.roll(jnp.where(lane == width - 1, pltpu.roll(left_rim, back, 1), block), 1, 1)
        right = pltpu.roll(jnp.where(lane == 0, pltpu.roll(right_rim, back, 1), block), width - 1, 1)
        return left, right

    def forward_row(state, rim, i):
        v, before, after = state[i + 1], state[i], state[i + 2]
        left, right = sides(v, rim[0], rim[1], i)
        s = spread[...]
        flow = (1.0 - 4.0 * s - ax[i + 1] - by[i]) * v + ax[i] * before + by_low[i] * left
        return flow + s * (before + after + left + right)

    def adjoint_row(state, rim, i):
        w, before, after = state[i + 1], state[i], state[i + 2]
        left, right = sides(w, rim[0], rim[1], i)
        s = spread[...]
        a, b = ax[i + 1], by[i]
        flow = (1.0 - 4.0 * s - a - b) * w + a * after + b * right
        return flow + s * (before + after + left + right)

    def rim_parts(block):
        return (
            pltpu.roll(block, GROUP, 1), pltpu.roll(block, width - GROUP, 1),
            pltpu.roll(block, 1, 1), pltpu.roll(block, width - 1, 1),
        )

    def forward_rim(block, side):
        before, after, left, right = rim_parts(block)
        s, a, b = spread[...], pa[0, side], pb[0, side]
        flow = (1.0 - 4.0 * s - a - b) * block
        flow = flow + pltpu.roll(a, GROUP, 1) * before + pltpu.roll(b, 1, 1) * left
        return jnp.where(inside[side], flow + s * (before + after + left + right), 0.0)

    def adjoint_rim(block, side):
        before, after, left, right = rim_parts(block)
        s, a, b = spread[...], pa[0, side], pb[0, side]
        flow = (1.0 - 4.0 * s - a - b) * block + a * after + b * right
        return jnp.where(inside[side], flow + s * (before + after + left + right), 0.0)

    def advance_rim(ref, n, rule, mats):
        both = mixed(mats, [rule(ref[n, 0], 0), rule(ref[n, 1], 1)])
        ref[n + 1, 0], ref[n + 1, 1] = both

    def forward_quad(n, q):
        which = quad_rows(q)
        values = mixed(mat, [forward_row(chain[0][n], (pv[n, 0], pv[n, 1]), i) for i in which])
        for i, value in zip(which, values):
            if n == STEPS - 1:
                end[i] = value
            else:
                chain[0][n + 1][i + 1] = value

    def adjoint_quad(n, q):
        which = quad_rows(q)
        values = mixed(mat_t, [adjoint_row(chain[1][n], (pw[n, 0], pw[n, 1]), i) for i in which])
        for i, value in zip(which, values):
            chain[1][n + 1][i + 1] = value

    def enter(q):
        which = quad_rows(q)
        arrived(u_recv, q)
        values = mixed(mat_t, [inbox[i] for i in which])
        for i, value in zip(which, values):
            w0[i + 1] = value
        pack_into(q_dual, 0, which, lambda i: inbox[i])

    def finish(out, which, values):
        squares = functools.reduce(jnp.add, [value * value for value in values])
        for i, value in zip(which, values):
            out[pl.ds(i, levels, stride=rows), :] = value
        acc[...] += squares

    def finish_dual(q, earlier):
        which = quad_rows(q)
        if earlier:
            arrived(e_recv, q)
        finish(out_dual, which, [forcing_v[i] + end_in[i] if earlier else forcing_v[i] for i in which])

    def early_residuals(i):
        d, v = dual_v[i], v0[i + 1]
        forcing_v[i] = forcing_v[i] - error_v[i] * d - v
        gradient_v[i] = gradient_v[i] - obs_v[i] * v - d

    @pl.when(has_prev)
    def _():
        send_quad(dual_copy, quads - 1)
        loaded(3)
        pack_into(q_own, 3, range(rows), lambda i: dual_v[i])
        start_both(q_up(3), q_down(3), y_first, y_last)
        heard_both(q_up(3), q_down(3), y_first, y_last)
        out_send[...] = jnp.where(near, q_left[3], q_right[3])
        send_quad(dual_copy, quads - 2)
        outside_copy().start()
        loop(quads - 2, lambda t: send_quad(dual_copy, quads - 3 - t))

    @pl.when(has_next)
    def _():
        x_start(0, 0)
        pl.when(not_(x_last))(lambda: a_up().start())
        for n, (f, value) in enumerate(
            ((0, lambda i: v0[i + 1]), (1, lambda i: by[i]), (2, lambda i: ax[i + 1]))
        ):
            loaded(f)
            pack_into(q_own, n, range(rows), value)
            start_both(q_up(n), q_down(n), y_first, y_last)

    pl.when(not_(has_next))(lambda: loaded(0, 1, 2))
    for line, semaphore in ((lines[1], met.at[0]),):
        greet(semaphore, line)

    @pl.when(has_next)
    def _():
        for n, ref in enumerate((pv, pb, pa)):
            heard_both(q_up(n), q_down(n), y_first, y_last)
            assemble(ref, 0, q_own[n], q_left[n], q_right[n])
        write_message(0, [ref[0, side] for ref in (pv, pb, pa) for side in (0, 1)])

        def lower(i):
            back = (2 * width - turn(i)) % width
            return pltpu.roll(jnp.where(lane == width - 1, pltpu.roll(pb[0, 0], back, 1), by[i]), 1, 1)

        def lower_four(t):
            four = [4 * t + j for j in range(4)]
            for i, value in zip(four, [lower(i) for i in four]):
                by_low[i] = value

        loop(rows // 4, lower_four)
        for q in range(quads - 1):
            forward_quad(0, q)
        x_heard(0, 0)
        pl.when(not_(x_first))(lambda: a_up().wait_recv())
        forward_quad(0, quads - 1)
        x_start(0, 1)
        advance_rim(pv, 0, forward_rim, mat)
        for q in range(quads - 1):
            forward_quad(1, q)
        advance_rim(pv, 1, forward_rim, mat)

        def early_end(q):
            forward_quad(2, q)
            send_quad(end_copy, q)

        for q in range(quads - 2):
            early_end(q)

        read_message(0, [(ref, 0, side) for ref in (pv, pb, pa) for side in (0, 1)])
        advance_rim(pv, 0, forward_rim, mat)
        x_heard(0, 1)
        forward_quad(1, quads - 1)
        x_start(0, 2)
        advance_rim(pv, 1, forward_rim, mat)
        early_end(quads - 2)

    for f in range(3, FIELDS):
        if f == 3:
            pl.when(not_(has_prev))(lambda: loaded(3))
        else:
            loaded(f)
    loop(rows, early_residuals)

    @pl.when(not_(has_prev))
    def _():
        loop(quads, lambda q: finish_dual(q, False))

    pl.semaphore_wait(met.at[0], nx - 1)
    greet(met.at[1], lines[0])

    @pl.when(has_next)
    def _():
        enter(quads - 1)
        x_start(1, 0)
        outside_copy().wait_recv()
        own, far = q_dual[0], outside[...]
        assemble(pu, 0, own, far, far)
        write_message(1, [pu[0, 0], pu[0, 1]])
        x_heard(0, 2)
        forward_quad(2, quads - 1)
        send_quad(end_copy, quads - 1)

        def enter_rim():
            own, far = q_dual[0], outside[...]
            both = []
            for side, (left, right) in enumerate(((far, own), (own, far))):
                value = jnp.where(near, left, right)
                low = pltpu.roll(x_msg_up[1], (-2 * GROUP * side) % width, 1)
                high = pltpu.roll(x_msg_down[1], (GROUP * (rows + 2) - 2 * GROUP * side) % width, 1)
                value = jnp.where(place < 0, low, jnp.where(place >= rows, high, value))
                both.append(jnp.where(inside[side], value, 0.0))
            pw[0, 0], pw[0, 1] = mixed(mat_t, both)

        def adjoint_quads(n, which):
            for q in which:
                if q == quads - 1:
                    x_heard(1, n)
                adjoint_quad(n, q)
                if q == quads - 1:
                    x_start(1, n + 1)

        for q in range(quads - 2, 0, -1):
            enter(q)
        heard_both(m_up(1), m_down(1), x_first, x_last)
        enter_rim()
        adjoint_quads(0, range(quads - 1, 1, -1))
        advance_rim(pw, 0, adjoint_rim, mat_t)
        adjoint_quads(1, range(quads - 1, 2, -1))
        enter(0)
        enter_rim()
        adjoint_quads(0, range(min(1, quads - 1), -1, -1))
        advance_rim(pw, 0, adjoint_rim, mat_t)
        adjoint_quads(1, range(min(2, quads - 1), -1, -1))
        advance_rim(pw, 1, adjoint_rim, mat_t)
        x_heard(1, 2)
        for q in range(quads):
            which = quad_rows(q)
            finish(
                out_incr, which,
                [gradient_v[i] + adjoint_row(w2, (pw[2, 0], pw[2, 1]), i) for i in which],
            )

    @pl.when(not_(has_next))
    def _():
        def body(q):
            which = quad_rows(q)
            finish(out_incr, which, [gradient_v[i] for i in which])

        loop(quads, body)

    pl.when(has_prev)(lambda: loop(quads, lambda q: finish_dual(q, True)))

    pl.semaphore_wait(met.at[1], windows - 1)
    part[...] = jnp.sum(acc[...], axis=0, keepdims=True)
    parts[me] = part[...]

    def coords(flat):
        return {"tm": flat // (nx * ny), "gx": (flat // ny) % nx, "gy": flat % ny}

    def tell(d):
        other = (me + d) % count
        return remote(part, parts.at[me], r_send, r_recv, coords(other))

    loop(count, lambda d: tell(d).start(), 1)

    pl.when(has_prev)(lambda: left_all(u_send))

    @pl.when(has_prev)
    def _():
        outside_copy().wait_send()
        sent_both(q_up(3), q_down(3), y_first, y_last)

    @pl.when(has_next)
    def _():
        left_all(e_send)
        pl.when(not_(x_last))(lambda: a_up().wait_send())
        for n in range(STEPS):
            sent_both(x_up(0, n), x_down(0, n), x_first, x_last)
            sent_both(x_up(1, n), x_down(1, n), x_first, x_last)
            sent_both(q_up(n), q_down(n), y_first, y_last)
        for n in range(2):
            sent_both(m_up(n), m_down(n), x_first, x_last)

    others = parts.at[pl.ds(0, count - 1)]
    every = remote(others, others, r_send, r_recv, {"tm": k})
    every.wait_recv()
    total = jnp.sum(jnp.sum(parts[...], axis=0), axis=1, keepdims=True)
    cells = 2 * rows * levels * width * count
    root_mean = jnp.sqrt(total / cells + 1e-06)
    out_scale[...] = jnp.broadcast_to(jnp.minimum(1.0, 0.5 / root_mean), out_scale.shape)
    every.wait_send()


def update(scale, dual, increment, residual_dual, residual_incr, dual_next, incr_next, dual_v, incr_v, sem):
    size = dual.shape[0]
    chunk = -(-size // (4 * 8)) * 8
    copies = []
    for lot, start in enumerate(range(0, size, chunk)):
        span = pl.ds(start, min(chunk, size - start))
        for j, (now, rest, home, out) in enumerate((
            (dual, residual_dual, dual_v, dual_next), (increment, residual_incr, incr_v, incr_next)
        )):
            home[span, :] = now[span, :] + scale[...] * rest[span, :]
            copies.append(pltpu.make_async_copy(home.at[span], out.at[span], sem.at[j, lot]))
            copies[-1].start()
    for copy in copies:
        copy.wait()


def local(axes, increment, dual_state, forcing, gradient, courant_x, courant_y, error_var, obs_weight, diffusion, level_mix):
    levels, rows, width = increment.shape[1:]
    count = axes[0] * axes[1] * axes[2]
    stack = -(-levels // 16) * 16
    assert rows % 4 == 0 and GROUP * (rows + 4) <= width
    fields = [
        part.reshape(levels, rows, 1, width)
        for part in (increment, dual_state, forcing, gradient, courant_x, courant_y, error_var, obs_weight)
    ]
    fields = [pltpu.with_memory_space_constraint(part, pltpu.HBM) for part in fields]
    slab = lambda *lead: pltpu.VMEM((*lead, levels, width), jnp.float32)
    dma = lambda *shape: pltpu.SemaphoreType.DMA(shape)
    one = pltpu.SemaphoreType.DMA
    scratch = [
        *[slab(rows + 2)] * 6, slab(rows + 1), slab(rows), slab(rows), slab(rows), slab(rows), slab(rows),
        slab(4), slab(4), slab(4), slab(), slab(1), slab(), slab(2, 2), slab(2), slab(2),
        slab(3, 2), slab(1, 2), slab(3, 2), slab(1, 2), slab(1, 2),
        slab(rows), slab(rows), slab(rows), slab(rows), slab(rows),
        slab(), pltpu.VMEM((levels, levels), jnp.float32), pltpu.VMEM((1, levels), jnp.float32),
        pltpu.VMEM((2 * stack, levels), jnp.bfloat16), pltpu.VMEM((2 * stack, levels), jnp.bfloat16),
        slab(), pltpu.VMEM((1, width), jnp.float32), pltpu.VMEM((count, 1, width), jnp.float32),
        dma(FIELDS), dma(2), one, dma(rows // 4), one, dma(rows // 4), dma(2),
        dma(2, STEPS, 2), dma(2, STEPS, 2), one, one, dma(4, 2), dma(4, 2), dma(2, 2), dma(2, 2),
        one, one, pltpu.SemaphoreType.REGULAR((2,)),
    ]
    field = jax.ShapeDtypeStruct((levels * rows, width), jnp.float32)
    vmem = pl.BlockSpec(memory_space=pltpu.VMEM)
    anywhere = pl.BlockSpec(memory_space=pltpu.HBM)
    residual_dual, residual_incr, scale = pl.pallas_call(
        functools.partial(kernel, axes),
        out_shape=(field, field, jax.ShapeDtypeStruct((1, width), jnp.float32)),
        in_specs=[anywhere] * 10,
        out_specs=(vmem, vmem, vmem),
        scratch_shapes=scratch,
        compiler_params=pltpu.CompilerParams(
            collective_id=0, has_side_effects=True, vmem_limit_bytes=32 * 1024 * 1024
        ),
    )(*fields, *(pltpu.with_memory_space_constraint(part, pltpu.HBM) for part in (diffusion[None, :], level_mix)))
    flat = lambda part: part.reshape(levels * rows, width)
    results = pl.pallas_call(
        update,
        out_shape=(field, field),
        in_specs=[vmem] * 5,
        out_specs=(anywhere, anywhere),
        scratch_shapes=[pltpu.VMEM(field.shape, jnp.float32)] * 2 + [dma(2, 4)],
        compiler_params=pltpu.CompilerParams(vmem_limit_bytes=16 * 1024 * 1024),
    )(scale, flat(dual_state), flat(increment), residual_dual, residual_incr)
    return tuple(part.reshape(increment.shape) for part in results)


def solution(mesh):
    spec = P("tm", None, "gx", "gy")
    axes = tuple(mesh.shape[name] for name in ("tm", "gx", "gy"))
    return jax.shard_map(
        functools.partial(local, axes),
        mesh=mesh,
        in_specs=(spec,) * FIELDS + (P(), P()),
        out_specs=(spec, spec),
        check_vma=False,
    )
```

```python
import functools

import jax
import jax.numpy as jnp
from jax import lax
from jax.experimental import pallas as pl
from jax.experimental.pallas import tpu as pltpu
from jax.sharding import PartitionSpec as P

STEPS = 3
MESH = pl.DeviceIdType.MESH
FIELDS = 8
RIM = STEPS
GROUP = 2 * RIM


def split(block):
    high = block.astype(jnp.bfloat16)
    return high, (block - high.astype(jnp.float32)).astype(jnp.bfloat16)


def kernel(
    axes,
    increment, dual, forcing, gradient, courant_x, courant_y, error_var, obs_weight, spread_row, matrix,
    out_dual, out_incr, out_scale,
    v0, v1, v2, w0, w1, w2, ax, by, inbox, end, end_in,
    q_own, q_left, q_right, outside, q_dual, out_send, x_msg, x_msg_up, x_msg_down,
    pv, pu, pw, pa, pb,
    dual_v, forcing_v, gradient_v, error_v, obs_v, spread, mat_v, spread_v, mat, mat_t, x_high, x_low, acc, part, parts,
    load_sem, small_sem, u_send, u_recv, e_send, e_recv, o_sem,
    x_send, x_recv, c_send, c_recv, q_send, q_recv, m_send, m_recv, r_send, r_recv, met,
):
    windows, nx, ny = axes
    count = windows * nx * ny
    rows, levels, width = dual_v.shape
    reach = rows // 2
    spans = [slice(low, min(low + 16, levels)) for low in range(0, levels, 16)]
    stack = mat.shape[0] // 2
    k, gx, gy = lax.axis_index("tm"), lax.axis_index("gx"), lax.axis_index("gy")
    me = (k * nx + gx) * ny + gy
    has_next, has_prev = k < windows - 1, k > 0
    not_ = jnp.logical_not
    x_first, x_last = gx == 0, gx == nx - 1
    y_first, y_last = gy == 0, gy == ny - 1
    lane = lax.broadcasted_iota(jnp.int32, (levels, width), 1)
    place = lane // GROUP - 2
    column = lane - (lane // GROUP) * GROUP
    near = column < RIM

    def remote(src, dst, send, recv, where):
        return pltpu.make_async_remote_copy(
            src_ref=src, dst_ref=dst, send_sem=send, recv_sem=recv, device_id=where, device_id_type=MESH
        )

    def loop(n, body, start=0):
        def step(i, carry):
            body(i)
            return carry

        lax.fori_loop(start, n, step, 0)

    homes = (
        (increment, lambda i: v0.at[i + 1]),
        (courant_y, lambda i: by.at[i]),
        (courant_x, lambda i: ax.at[i + 1]),
        (dual, lambda i: dual_v.at[i]),
        (forcing, lambda i: forcing_v.at[i]),
        (gradient, lambda i: gradient_v.at[i]),
        (error_var, lambda i: error_v.at[i]),
        (obs_weight, lambda i: obs_v.at[i]),
    )

    def load(f, i):
        source, home = homes[f]
        return pltpu.make_async_copy(source.at[:, i, 0], home(i), load_sem.at[f])

    def loaded(*which):
        for f in which:
            pltpu.make_async_copy(homes[f][0], homes[f][0], load_sem.at[f]).wait()

    barrier = pltpu.get_barrier_semaphore()
    lines = (("tm", k, windows), ("gx", gx, nx), ("gy", gy, ny))

    def greet(semaphore, line):
        name, mine, size = line
        for d in range(1, size):
            other = lax.rem(mine + d, size)
            pl.semaphore_signal(semaphore, inc=1, device_id={name: other}, device_id_type=MESH)

    for line in lines:
        greet(barrier, line)

    small = (
        pltpu.make_async_copy(spread_row, spread_v, small_sem.at[0]),
        pltpu.make_async_copy(matrix, mat_v, small_sem.at[1]),
    )
    for copy in small:
        copy.start()
    for f in range(FIELDS):
        loop(rows, lambda i, f=f: load(f, i).start())

    for copy in small:
        copy.wait()
    spread[...] = jnp.swapaxes(jnp.broadcast_to(spread_v[...], (width, levels)), 0, 1)
    for source, home in ((mat_v[...], mat), (jnp.swapaxes(mat_v[...], 0, 1), mat_t)):
        high, low = split(source)
        home[0:levels, :] = high
        home[stack : stack + levels, :] = low
    acc[...] = jnp.zeros_like(acc)
    zero = jnp.zeros((levels, width), jnp.float32)

    @pl.when(x_first)
    def _():
        ax[0] = zero
        for state in (v0, v1, v2, w0, w1, w2):
            state[0] = zero

    @pl.when(x_last)
    def _():
        for state in (v0, v1, v2, w0, w1, w2):
            state[rows + 1] = zero

    pl.semaphore_wait(barrier, windows + nx + ny - 3)

    def mirror(*steps):
        return [i for j in steps for i in (reach - 1 - j, reach + j)]

    def paired(steps):
        steps = list(steps)
        return [steps[t : t + 2] for t in range(0, len(steps), 2)]

    outward = [[0]] + paired(range(1, reach))
    inward = paired(range(reach - 1, 1, -1)) + [[1], [0]]

    def arrived(semaphores, lot, size):
        whole = dual.at[:, pl.ds(0, size)]
        remote(whole, whole, u_send, semaphores.at[lot], {"tm": k}).wait_recv()

    def left_all(semaphore):
        remote(dual, dual, semaphore, u_recv.at[0], {"tm": k}).wait_send()

    def dual_copy(i, q):
        return remote(dual.at[:, i, 0], inbox.at[i], u_send, u_recv.at[q], {"tm": k - 1})

    def end_copy(i, q):
        return remote(end.at[i], end_in.at[i], e_send, e_recv.at[q], {"tm": k + 1})

    def outside_copy():
        return remote(out_send, outside, o_sem.at[0], o_sem.at[1], {"tm": k - 1})

    def send_duals(lots):
        for lot in lots:
            for i in mirror(*inward[lot]):
                dual_copy(i, lot).start()

    chain = ((v0, v1, v2), (w0, w1, w2))

    def x_up(c, n):
        state = chain[c][n]
        src = increment.at[:, rows - 1, 0] if (c, n) == (0, 0) else state.at[rows]
        return remote(src, state.at[0], x_send.at[c, n, 0], x_recv.at[c, n, 0], {"gx": gx + 1})

    def x_down(c, n):
        state = chain[c][n]
        src = increment.at[:, 0, 0] if (c, n) == (0, 0) else state.at[1]
        return remote(src, state.at[rows + 1], x_send.at[c, n, 1], x_recv.at[c, n, 1], {"gx": gx - 1})

    def a_up():
        return remote(courant_x.at[:, rows - 1, 0], ax.at[0], c_send, c_recv, {"gx": gx + 1})

    def m_up(n):
        return remote(x_msg.at[n, 0], x_msg_up.at[n], m_send.at[n, 0], m_recv.at[n, 0], {"gx": gx + 1})

    def m_down(n):
        return remote(x_msg.at[n, 1], x_msg_down.at[n], m_send.at[n, 1], m_recv.at[n, 1], {"gx": gx - 1})

    def q_up(n):
        return remote(q_own.at[n], q_left.at[n], q_send.at[n, 0], q_recv.at[n, 0], {"gy": gy + 1})

    def q_down(n):
        return remote(q_own.at[n], q_right.at[n], q_send.at[n, 1], q_recv.at[n, 1], {"gy": gy - 1})

    def start_both(up, down, first, last):
        pl.when(not_(last))(lambda: up.start())
        pl.when(not_(first))(lambda: down.start())

    def heard_both(up, down, first, last):
        pl.when(not_(first))(lambda: up.wait_recv())
        pl.when(not_(last))(lambda: down.wait_recv())

    def sent_both(up, down, first, last):
        pl.when(not_(last))(lambda: up.wait_send())
        pl.when(not_(first))(lambda: down.wait_send())

    def x_start(c, n):
        start_both(x_up(c, n), x_down(c, n), x_first, x_last)

    def x_heard(c, n):
        heard_both(x_up(c, n), x_down(c, n), x_first, x_last)

    def turn(i):
        return GROUP * (i + 2) + RIM

    def pack_into(ref, index, which, value):
        for lv in spans:
            packed = ref[index, lv]
            for i in which:
                packed = jnp.where(place[lv] == i, pltpu.roll(value(i, lv), turn(i) % width, 1), packed)
            ref[index, lv] = packed

    inside_x = ((place >= 0) | not_(x_first)) & ((place < rows) | not_(x_last)) & (place < rows + 2)
    own_rows = (place >= 0) & (place < rows)
    inside = (
        inside_x & (not_(near) | not_(y_first)),
        inside_x & (near | not_(y_last)),
    )

    def assemble(target, index, own, left, right):
        target[index, 0] = jnp.where(inside[0] & own_rows, jnp.where(near, left, own), 0.0)
        target[index, 1] = jnp.where(inside[1] & own_rows, jnp.where(near, own, right), 0.0)

    def write_message(n, blocks):
        up, down = zero, zero
        for b, block in enumerate(blocks):
            mine = lane // (2 * GROUP) == b
            up = jnp.where(mine, pltpu.roll(block, (2 * GROUP * b - GROUP * rows) % width, 1), up)
            down = jnp.where(mine, pltpu.roll(block, (2 * GROUP * b - 2 * GROUP) % width, 1), down)
        x_msg[n, 0] = up
        x_msg[n, 1] = down
        start_both(m_up(n), m_down(n), x_first, x_last)

    def read_message(n, refs):
        heard_both(m_up(n), m_down(n), x_first, x_last)
        for b, (ref, index, side) in enumerate(refs):
            low = pltpu.roll(x_msg_up[n], (-2 * GROUP * b) % width, 1)
            high = pltpu.roll(x_msg_down[n], (GROUP * (rows + 2) - 2 * GROUP * b) % width, 1)
            value = jnp.where(place < 0, low, jnp.where(place >= rows, high, ref[index, side]))
            ref[index, side] = jnp.where(inside[side], value, 0.0)

    turns = [0]

    def mixed(mats, rule, size, put):
        turns[0] = 1 - turns[0]
        highs, lows = x_high.at[turns[0]], x_low.at[turns[0]]
        for lv in spans:
            for j, value in enumerate(rule(lv)):
                highs[lv, j * width : (j + 1) * width], lows[lv, j * width : (j + 1) * width] = split(value)
        dot = functools.partial(jnp.dot, preferred_element_type=jnp.float32)
        top, rest = mats.at[0:levels], mats.at[stack : stack + levels]
        for j in range(0, size, 2):
            here = slice(j * width, (j + 2) * width)
            result = dot(top[...], lows[:, here]) + dot(rest[...], highs[:, here]) + dot(top[...], highs[:, here])
            put(j, result[:, :width])
            put(j + 1, result[:, width:])

    def back(i):
        return (2 * width - turn(i)) % width

    def from_left(block, rim, i, lv):
        return pltpu.roll(jnp.where(lane[lv] == width - 1, pltpu.roll(rim, back(i), 1), block), 1, 1)

    def from_right(block, rim, i, lv):
        return pltpu.roll(jnp.where(lane[lv] == 0, pltpu.roll(rim, back(i), 1), block), width - 1, 1)

    def forward_rows(n, which, lv):
        state, s = chain[0][n], spread[lv]
        keep = 1.0 - 4.0 * s
        values = []
        for i in which:
            v, before, after = state[i + 1, lv], state[i, lv], state[i + 2, lv]
            b = by[i, lv]
            left = from_left((b + s) * v, (pb[0, 0, lv] + s) * pv[n, 0, lv], i, lv)
            right = from_right(v, pv[n, 1, lv], i, lv)
            flow = (keep - ax[i + 1, lv] - b) * v + ax[i, lv] * before + left
            values.append(flow + s * (before + after + right))
        return values

    def adjoint_rows(n, which, lv):
        state, s = chain[1][n], spread[lv]
        keep = 1.0 - 4.0 * s
        values = []
        for i in which:
            w, before, after = state[i + 1, lv], state[i, lv], state[i + 2, lv]
            left = from_left(w, pw[n, 0, lv], i, lv)
            right = from_right(w, pw[n, 1, lv], i, lv)
            a, b = ax[i + 1, lv], by[i, lv]
            flow = (keep - a - b) * w + a * after + b * right
            values.append(flow + s * (before + after + left + right))
        return values

    def rim_parts(block):
        return (
            pltpu.roll(block, GROUP, 1), pltpu.roll(block, width - GROUP, 1),
            pltpu.roll(block, 1, 1), pltpu.roll(block, width - 1, 1),
        )

    def forward_rim(block, side, lv):
        before, after, left, right = rim_parts(block)
        s, a, b = spread[lv], pa[0, side, lv], pb[0, side, lv]
        flow = (1.0 - 4.0 * s - a - b) * block
        flow = flow + pltpu.roll(a, GROUP, 1) * before + pltpu.roll(b, 1, 1) * left
        return jnp.where(inside[side][lv], flow + s * (before + after + left + right), 0.0)

    def adjoint_rim(block, side, lv):
        before, after, left, right = rim_parts(block)
        s, a, b = spread[lv], pa[0, side, lv], pb[0, side, lv]
        flow = (1.0 - 4.0 * s - a - b) * block + a * after + b * right
        return jnp.where(inside[side][lv], flow + s * (before + after + left + right), 0.0)

    def put_all(state, shift, which, rims=None, n=0):
        def put(j, value):
            if j < len(which):
                state[which[j] + shift] = value
            else:
                rims[n, j - len(which)] = value

        return put

    def advance_rim(ref, n, rule, mats):
        mixed(mats, lambda lv: [rule(ref[n, side, lv], side, lv) for side in (0, 1)], 2, put_all(None, 0, [], ref, n + 1))

    def forward(n, steps, rim):
        which = mirror(*steps)
        target = (end, 0) if n == STEPS - 1 else (chain[0][n + 1], 1)

        def rule(lv):
            return forward_rows(n, which, lv) + [forward_rim(pv[n, side, lv], side, lv) for side in (0, 1) if rim]

        mixed(mat, rule, len(which) + 2 * rim, put_all(*target, which, pv, n + 1))

    def adjoint(n, steps, rim):
        which = mirror(*steps)
        if n == STEPS - 1:
            def body(t):
                pair = mirror(steps[0] - t)
                finish(out_incr, pair, lambda lv: [
                    gradient_v[i, lv] + value for i, value in zip(pair, adjoint_rows(n, pair, lv))
                ])

            loop(len(steps), body)
        else:
            def rule(lv):
                return adjoint_rows(n, which, lv) + [adjoint_rim(pw[n, side, lv], side, lv) for side in (0, 1) if rim]

            mixed(mat_t, rule, len(which) + 2 * rim, put_all(chain[1][n + 1], 1, which, pw, n + 1))

    def rim_entry(lv):
        own, far = q_dual[0, lv], outside[lv]
        both = []
        for side, (left, right) in enumerate(((far, own), (own, far))):
            value = jnp.where(near[lv], left, right)
            low = pltpu.roll(x_msg_up[1, lv], (-2 * GROUP * side) % width, 1)
            high = pltpu.roll(x_msg_down[1, lv], (GROUP * (rows + 2) - 2 * GROUP * side) % width, 1)
            value = jnp.where(place[lv] < 0, low, jnp.where(place[lv] >= rows, high, value))
            both.append(jnp.where(inside[side][lv], value, 0.0))
        return both

    def enter(lot):
        which = mirror(*inward[lot])
        arrived(u_recv, lot, len(which))
        pack_into(q_dual, 0, which, lambda i, lv: inbox[i, lv])
        if lot == 1:
            heard_both(m_up(1), m_down(1), x_first, x_last)
        rim = lot > 0

        def rule(lv):
            return [inbox[i, lv] for i in which] + (rim_entry(lv) if rim else [])

        mixed(mat_t, rule, len(which) + 2 * rim, put_all(w0, 1, which, pw, 0))

    done = [0] * STEPS

    def produce(n, steps):
        if n:
            while done[n - 1] < min(steps[-1] + 2, reach):
                first = done[n - 1]
                produce(n - 1, range(first, min(first + 2, reach)))
        edge = steps[-1] == reach - 1
        if edge:
            if n == 0:
                write_message(0, [ref[0, side] for ref in (pv, pb, pa) for side in (0, 1)])
                pl.when(not_(x_first))(lambda: a_up().wait_recv())
            if n == 1:
                read_message(0, [(ref, 0, side) for ref in (pv, pb, pa) for side in (0, 1)])
            x_heard(0, n)
        if n == 1 and edge:
            advance_rim(pv, 0, forward_rim, mat)
        first = done[n]
        done[n] += len(steps)
        rim = (n == 0 and first < 3 <= done[n]) or (n == 1 and (first == 0 or edge))
        forward(n, steps, False)
        if rim:
            advance_rim(pv, n, forward_rim, mat)
        if edge and n < STEPS - 1:
            x_start(0, n + 1)

    def produce_end(lot):
        produce(STEPS - 1, outward[lot])
        for i in mirror(*outward[lot]):
            end_copy(i, lot).start()

    def finish(out, which, values):
        sums = {}
        for lv in spans:
            size = lv.stop - lv.start
            for i, value in zip(which, values(lv)):
                out[pl.ds(lv.start * rows + i, size, stride=rows), :] = value
                sums[size] = sums[size] + value * value if size in sums else value * value
        for size, value in sums.items():
            acc[0:size] += value

    def finish_dual(lot, earlier):
        if earlier:
            arrived(e_recv, lot, 2 * len(outward[lot]))

        def body(t):
            pair = mirror(outward[lot][0] + t)
            finish(out_dual, pair, lambda lv: [
                forcing_v[i, lv] + end_in[i, lv] if earlier else forcing_v[i, lv] for i in pair
            ])

        loop(len(outward[lot]), body)

    def early_residuals(i):
        d, v = dual_v[i], v0[i + 1]
        forcing_v[i] = forcing_v[i] - error_v[i] * d - v
        gradient_v[i] = gradient_v[i] - obs_v[i] * v - d

    @pl.when(has_prev)
    def _():
        send_duals([0])
        loaded(3)
        pack_into(q_own, 3, range(rows), lambda i, lv: dual_v[i, lv])
        start_both(q_up(3), q_down(3), y_first, y_last)
        heard_both(q_up(3), q_down(3), y_first, y_last)
        out_send[...] = jnp.where(near, q_left[3], q_right[3])
        outside_copy().start()
        send_duals(range(1, len(inward)))

    @pl.when(has_next)
    def _():
        x_start(0, 0)
        pl.when(not_(x_last))(lambda: a_up().start())
        for n, (f, value) in enumerate(
            ((0, lambda i, lv: v0[i + 1, lv]), (1, lambda i, lv: by[i, lv]), (2, lambda i, lv: ax[i + 1, lv]))
        ):
            loaded(f)
            pack_into(q_own, n, range(rows), value)
            start_both(q_up(n), q_down(n), y_first, y_last)

    pl.when(not_(has_next))(lambda: loaded(0, 1, 2))
    for line, semaphore in ((lines[1], met.at[0]),):
        greet(semaphore, line)

    @pl.when(has_next)
    def _():
        for n, ref in enumerate((pv, pb, pa)):
            heard_both(q_up(n), q_down(n), y_first, y_last)
            assemble(ref, 0, q_own[n], q_left[n], q_right[n])
        for lot in range(len(outward) - 2):
            produce_end(lot)

    for f in range(3, FIELDS):
        if f == 3:
            pl.when(not_(has_prev))(lambda: loaded(3))
        else:
            loaded(f)
    loop(rows, early_residuals)

    @pl.when(not_(has_prev))
    def _():
        for lot in range(len(outward)):
            finish_dual(lot, False)

    pl.semaphore_wait(met.at[0], nx - 1)
    greet(met.at[1], lines[0])

    @pl.when(has_next)
    def _():
        enter(0)
        x_start(1, 0)
        produce_end(len(outward) - 2)
        outside_copy().wait_recv()
        own, far = q_dual[0], outside[...]
        assemble(pu, 0, own, far, far)
        write_message(1, [pu[0, 0], pu[0, 1]])
        floor = [reach] * STEPS
        for lot in range(1, len(inward)):
            enter(lot)
            least = inward[lot][-1]
            for n in range(min(lot, STEPS) if least else STEPS):
                low = least + 1 + n if least else 0
                lots = paired(range(floor[n] - 1, low - 1, -1))
                for t, steps in enumerate(lots):
                    edge = steps[0] == reach - 1
                    if edge:
                        x_heard(1, n)
                    adjoint(n, steps, t == len(lots) - 1)
                    if edge and n < STEPS - 1:
                        x_start(1, n + 1)
                floor[n] = min(floor[n], low)
            if lot == 1:
                produce_end(len(outward) - 1)

    @pl.when(not_(has_next))
    def _():
        for lot in range(len(outward)):
            def body(t):
                pair = mirror(outward[lot][0] + t)
                finish(out_incr, pair, lambda lv: [gradient_v[i, lv] for i in pair])

            loop(len(outward[lot]), body)

    @pl.when(has_prev)
    def _():
        for lot in range(len(outward)):
            finish_dual(lot, True)

    pl.semaphore_wait(met.at[1], windows - 1)
    part[...] = jnp.sum(acc[...], axis=0, keepdims=True)
    parts[me] = part[...]

    def coords(flat):
        return {"tm": flat // (nx * ny), "gx": (flat // ny) % nx, "gy": flat % ny}

    def tell(d):
        other = (me + d) % count
        return remote(part, parts.at[me], r_send, r_recv, coords(other))

    loop(count, lambda d: tell(d).start(), 1)

    pl.when(has_prev)(lambda: left_all(u_send))

    @pl.when(has_prev)
    def _():
        outside_copy().wait_send()
        sent_both(q_up(3), q_down(3), y_first, y_last)

    @pl.when(has_next)
    def _():
        left_all(e_send)
        pl.when(not_(x_last))(lambda: a_up().wait_send())
        for n in range(STEPS):
            sent_both(x_up(0, n), x_down(0, n), x_first, x_last)
            sent_both(x_up(1, n), x_down(1, n), x_first, x_last)
            sent_both(q_up(n), q_down(n), y_first, y_last)
        for n in range(2):
            sent_both(m_up(n), m_down(n), x_first, x_last)

    others = parts.at[pl.ds(0, count - 1)]
    every = remote(others, others, r_send, r_recv, {"tm": k})
    every.wait_recv()
    total = jnp.sum(jnp.sum(parts[...], axis=0), axis=1, keepdims=True)
    cells = 2 * rows * levels * width * count
    root_mean = jnp.sqrt(total / cells + 1e-06)
    out_scale[...] = jnp.broadcast_to(jnp.minimum(1.0, 0.5 / root_mean), out_scale.shape)
    every.wait_send()


def update(scale, dual, increment, residual_dual, residual_incr, dual_next, incr_next, dual_v, incr_v, sem):
    size = dual.shape[0]
    chunk = -(-size // (4 * 8)) * 8
    copies = []
    for lot, start in enumerate(range(0, size, chunk)):
        span = pl.ds(start, min(chunk, size - start))
        for j, (now, rest, home, out) in enumerate((
            (dual, residual_dual, dual_v, dual_next), (increment, residual_incr, incr_v, incr_next)
        )):
            for low in range(start, min(start + chunk, size), 64):
                piece = pl.ds(low, min(64, start + chunk - low, size - low))
                home[piece, :] = now[piece, :] + scale[...] * rest[piece, :]
            copies.append(pltpu.make_async_copy(home.at[span], out.at[span], sem.at[j, lot]))
            copies[-1].start()
    for copy in copies:
        copy.wait()


def local(axes, increment, dual_state, forcing, gradient, courant_x, courant_y, error_var, obs_weight, diffusion, level_mix):
    levels, rows, width = increment.shape[1:]
    count = axes[0] * axes[1] * axes[2]
    stack = -(-levels // 16) * 16
    reach = rows // 2
    assert rows % 4 == 0 and rows >= 8 and GROUP * (rows + 4) <= width
    fields = [
        part.reshape(levels, rows, 1, width)
        for part in (increment, dual_state, forcing, gradient, courant_x, courant_y, error_var, obs_weight)
    ]
    fields = [pltpu.with_memory_space_constraint(part, pltpu.HBM) for part in fields]
    slab = lambda *lead: pltpu.VMEM((*lead, levels, width), jnp.float32)
    dma = lambda *shape: pltpu.SemaphoreType.DMA(shape)
    one = pltpu.SemaphoreType.DMA
    scratch = [
        *[slab(rows + 2)] * 6, slab(rows + 1), slab(rows), slab(rows), slab(rows), slab(rows),
        slab(4), slab(4), slab(4), slab(), slab(1), slab(), slab(2, 2), slab(2), slab(2),
        slab(3, 2), slab(1, 2), slab(3, 2), slab(1, 2), slab(1, 2),
        slab(rows), slab(rows), slab(rows), slab(rows), slab(rows),
        slab(), pltpu.VMEM((levels, levels), jnp.float32), pltpu.VMEM((1, levels), jnp.float32),
        pltpu.VMEM((2 * stack, levels), jnp.bfloat16), pltpu.VMEM((2 * stack, levels), jnp.bfloat16),
        *[pltpu.VMEM((2, levels, 8 * width), jnp.bfloat16)] * 2,
        pltpu.VMEM((16, width), jnp.float32), pltpu.VMEM((1, width), jnp.float32), pltpu.VMEM((count, 1, width), jnp.float32),
        dma(FIELDS), dma(2), one, dma(reach), one, dma(reach), dma(2),
        dma(2, STEPS, 2), dma(2, STEPS, 2), one, one, dma(4, 2), dma(4, 2), dma(2, 2), dma(2, 2),
        one, one, pltpu.SemaphoreType.REGULAR((2,)),
    ]
    field = jax.ShapeDtypeStruct((levels * rows, width), jnp.float32)
    vmem = pl.BlockSpec(memory_space=pltpu.VMEM)
    anywhere = pl.BlockSpec(memory_space=pltpu.HBM)
    residual_dual, residual_incr, scale = pl.pallas_call(
        functools.partial(kernel, axes),
        out_shape=(field, field, jax.ShapeDtypeStruct((1, width), jnp.float32)),
        in_specs=[anywhere] * 10,
        out_specs=(vmem, vmem, vmem),
        scratch_shapes=scratch,
        compiler_params=pltpu.CompilerParams(
            collective_id=0, has_side_effects=True, vmem_limit_bytes=32 * 1024 * 1024
        ),
    )(*fields, *(pltpu.with_memory_space_constraint(part, pltpu.HBM) for part in (diffusion[None, :], level_mix)))
    flat = lambda part: part.reshape(levels * rows, width)
    results = pl.pallas_call(
        update,
        out_shape=(field, field),
        in_specs=[vmem] * 5,
        out_specs=(anywhere, anywhere),
        scratch_shapes=[pltpu.VMEM(field.shape, jnp.float32)] * 2 + [dma(2, 4)],
        compiler_params=pltpu.CompilerParams(vmem_limit_bytes=16 * 1024 * 1024),
    )(scale, flat(dual_state), flat(increment), residual_dual, residual_incr)
    return tuple(part.reshape(increment.shape) for part in results)


def solution(mesh):
    spec = P("tm", None, "gx", "gy")
    axes = tuple(mesh.shape[name] for name in ("tm", "gx", "gy"))
    return jax.shard_map(
        functools.partial(local, axes),
        mesh=mesh,
        in_specs=(spec,) * FIELDS + (P(), P()),
        out_specs=(spec, spec),
        check_vma=False,
    )
```

```python
import functools

import jax
import jax.numpy as jnp
from jax import lax
from jax.experimental import pallas as pl
from jax.experimental.pallas import tpu as pltpu
from jax.sharding import PartitionSpec as P

STEPS = 3
MESH = pl.DeviceIdType.MESH
FIELDS = 8
RIM = STEPS
GROUP = 2 * RIM


def split(block):
    high = block.astype(jnp.bfloat16)
    return high, (block - high.astype(jnp.float32)).astype(jnp.bfloat16)


def kernel(
    axes,
    increment, dual, forcing, gradient, courant_x, courant_y, error_var, obs_weight, spread_row, matrix,
    out_dual, out_incr, out_scale,
    v0, v1, v2, w0, w1, w2, ax, by, inbox, end, end_in,
    q_own, q_left, q_right, outside, q_dual, out_send, x_msg, x_msg_up, x_msg_down,
    pv, pu, pw, pa, pb,
    dual_v, forcing_v, gradient_v, error_v, obs_v, spread, mat_v, spread_v, mat, mat_t, x_high, x_low, acc, part, parts,
    load_sem, small_sem, u_send, u_recv, e_send, e_recv, o_sem,
    x_send, x_recv, c_send, c_recv, q_send, q_recv, m_send, m_recv, r_send, r_recv, met,
):
    windows, nx, ny = axes
    count = windows * nx * ny
    rows, levels, width = dual_v.shape
    reach = rows // 2
    spans = [slice(low, min(low + 16, levels)) for low in range(0, levels, 16)]
    stack = mat.shape[0] // 2
    k, gx, gy = lax.axis_index("tm"), lax.axis_index("gx"), lax.axis_index("gy")
    me = (k * nx + gx) * ny + gy
    has_next, has_prev = k < windows - 1, k > 0
    not_ = jnp.logical_not
    x_first, x_last = gx == 0, gx == nx - 1
    y_first, y_last = gy == 0, gy == ny - 1
    lane = lax.broadcasted_iota(jnp.int32, (levels, width), 1)
    place = lane // GROUP - 2
    column = lane - (lane // GROUP) * GROUP
    near = column < RIM

    def remote(src, dst, send, recv, where):
        return pltpu.make_async_remote_copy(
            src_ref=src, dst_ref=dst, send_sem=send, recv_sem=recv, device_id=where, device_id_type=MESH
        )

    def loop(n, body, start=0):
        def step(i, carry):
            body(i)
            return carry

        lax.fori_loop(start, n, step, 0)

    homes = (
        (increment, lambda i: v0.at[i + 1]),
        (courant_y, lambda i: by.at[i]),
        (courant_x, lambda i: ax.at[i + 1]),
        (dual, lambda i: dual_v.at[i]),
        (forcing, lambda i: forcing_v.at[i]),
        (gradient, lambda i: gradient_v.at[i]),
        (error_var, lambda i: error_v.at[i]),
        (obs_weight, lambda i: obs_v.at[i]),
    )

    def load(f, i):
        source, home = homes[f]
        return pltpu.make_async_copy(source.at[:, i, 0], home(i), load_sem.at[f])

    def loaded(*which):
        for f in which:
            pltpu.make_async_copy(homes[f][0], homes[f][0], load_sem.at[f]).wait()

    barrier = pltpu.get_barrier_semaphore()
    lines = (("tm", k, windows), ("gx", gx, nx), ("gy", gy, ny))

    def greet(semaphore, line):
        name, mine, size = line
        for d in range(1, size):
            other = lax.rem(mine + d, size)
            pl.semaphore_signal(semaphore, inc=1, device_id={name: other}, device_id_type=MESH)

    for line in lines:
        greet(barrier, line)

    small = (
        pltpu.make_async_copy(spread_row, spread_v, small_sem.at[0]),
        pltpu.make_async_copy(matrix, mat_v, small_sem.at[1]),
    )
    for copy in small:
        copy.start()
    for f in range(FIELDS):
        loop(rows, lambda i, f=f: load(f, i).start())

    for copy in small:
        copy.wait()
    spread[...] = jnp.swapaxes(jnp.broadcast_to(spread_v[...], (width, levels)), 0, 1)
    for source, home in ((mat_v[...], mat), (jnp.swapaxes(mat_v[...], 0, 1), mat_t)):
        high, low = split(source)
        home[0:levels, :] = high
        home[stack : stack + levels, :] = low
    acc[...] = jnp.zeros_like(acc)
    zero = jnp.zeros((levels, width), jnp.float32)

    @pl.when(x_first)
    def _():
        ax[0] = zero
        for state in (v0, v1, v2, w0, w1, w2):
            state[0] = zero

    @pl.when(x_last)
    def _():
        for state in (v0, v1, v2, w0, w1, w2):
            state[rows + 1] = zero

    with jax.named_scope('barrier'): pl.semaphore_wait(barrier, windows + nx + ny - 3)

    def mirror(*steps):
        return [i for j in steps for i in (reach - 1 - j, reach + j)]

    def paired(steps):
        steps = list(steps)
        return [steps[t : t + 2] for t in range(0, len(steps), 2)]

    outward = [[0]] + paired(range(1, reach))
    inward = paired(range(reach - 1, 1, -1)) + [[1], [0]]

    def arrived(semaphores, lot, size):
        whole = dual.at[:, pl.ds(0, size)]
        remote(whole, whole, u_send, semaphores.at[lot], {"tm": k}).wait_recv()

    def left_all(semaphore):
        remote(dual, dual, semaphore, u_recv.at[0], {"tm": k}).wait_send()

    def dual_copy(i, q):
        return remote(dual.at[:, i, 0], inbox.at[i], u_send, u_recv.at[q], {"tm": k - 1})

    def end_copy(i, q):
        return remote(end.at[i], end_in.at[i], e_send, e_recv.at[q], {"tm": k + 1})

    def outside_copy():
        return remote(out_send, outside, o_sem.at[0], o_sem.at[1], {"tm": k - 1})

    def send_duals(lots):
        for lot in lots:
            for i in mirror(*inward[lot]):
                dual_copy(i, lot).start()

    chain = ((v0, v1, v2), (w0, w1, w2))

    def x_up(c, n):
        state = chain[c][n]
        src = increment.at[:, rows - 1, 0] if (c, n) == (0, 0) else state.at[rows]
        return remote(src, state.at[0], x_send.at[c, n, 0], x_recv.at[c, n, 0], {"gx": gx + 1})

    def x_down(c, n):
        state = chain[c][n]
        src = increment.at[:, 0, 0] if (c, n) == (0, 0) else state.at[1]
        return remote(src, state.at[rows + 1], x_send.at[c, n, 1], x_recv.at[c, n, 1], {"gx": gx - 1})

    def a_up():
        return remote(courant_x.at[:, rows - 1, 0], ax.at[0], c_send, c_recv, {"gx": gx + 1})

    def m_up(n):
        return remote(x_msg.at[n, 0], x_msg_up.at[n], m_send.at[n, 0], m_recv.at[n, 0], {"gx": gx + 1})

    def m_down(n):
        return remote(x_msg.at[n, 1], x_msg_down.at[n], m_send.at[n, 1], m_recv.at[n, 1], {"gx": gx - 1})

    def q_up(n):
        return remote(q_own.at[n], q_left.at[n], q_send.at[n, 0], q_recv.at[n, 0], {"gy": gy + 1})

    def q_down(n):
        return remote(q_own.at[n], q_right.at[n], q_send.at[n, 1], q_recv.at[n, 1], {"gy": gy - 1})

    def start_both(up, down, first, last):
        pl.when(not_(last))(lambda: up.start())
        pl.when(not_(first))(lambda: down.start())

    def heard_both(up, down, first, last):
        pl.when(not_(first))(lambda: up.wait_recv())
        pl.when(not_(last))(lambda: down.wait_recv())

    def sent_both(up, down, first, last):
        pl.when(not_(last))(lambda: up.wait_send())
        pl.when(not_(first))(lambda: down.wait_send())

    def x_start(c, n):
        start_both(x_up(c, n), x_down(c, n), x_first, x_last)

    def x_heard(c, n):
        heard_both(x_up(c, n), x_down(c, n), x_first, x_last)

    def turn(i):
        return GROUP * (i + 2) + RIM

    def pack_into(ref, index, which, value):
        for lv in spans:
            packed = ref[index, lv]
            for i in which:
                packed = jnp.where(place[lv] == i, pltpu.roll(value(i, lv), turn(i) % width, 1), packed)
            ref[index, lv] = packed

    inside_x = ((place >= 0) | not_(x_first)) & ((place < rows) | not_(x_last)) & (place < rows + 2)
    own_rows = (place >= 0) & (place < rows)
    inside = (
        inside_x & (not_(near) | not_(y_first)),
        inside_x & (near | not_(y_last)),
    )

    def assemble(target, index, own, left, right):
        target[index, 0] = jnp.where(inside[0] & own_rows, jnp.where(near, left, own), 0.0)
        target[index, 1] = jnp.where(inside[1] & own_rows, jnp.where(near, own, right), 0.0)

    def write_message(n, blocks):
        up, down = zero, zero
        for b, block in enumerate(blocks):
            mine = lane // (2 * GROUP) == b
            up = jnp.where(mine, pltpu.roll(block, (2 * GROUP * b - GROUP * rows) % width, 1), up)
            down = jnp.where(mine, pltpu.roll(block, (2 * GROUP * b - 2 * GROUP) % width, 1), down)
        x_msg[n, 0] = up
        x_msg[n, 1] = down
        start_both(m_up(n), m_down(n), x_first, x_last)

    def read_message(n, refs):
        heard_both(m_up(n), m_down(n), x_first, x_last)
        for b, (ref, index, side) in enumerate(refs):
            low = pltpu.roll(x_msg_up[n], (-2 * GROUP * b) % width, 1)
            high = pltpu.roll(x_msg_down[n], (GROUP * (rows + 2) - 2 * GROUP * b) % width, 1)
            value = jnp.where(place < 0, low, jnp.where(place >= rows, high, ref[index, side]))
            ref[index, side] = jnp.where(inside[side], value, 0.0)

    turns = [0]

    def mixed(mats, rule, size, put):
        turns[0] = 1 - turns[0]
        highs, lows = x_high.at[turns[0]], x_low.at[turns[0]]
        for lv in spans:
            for j, value in enumerate(rule(lv)):
                highs[lv, j * width : (j + 1) * width], lows[lv, j * width : (j + 1) * width] = split(value)
        dot = functools.partial(jnp.dot, preferred_element_type=jnp.float32)
        top, rest = mats.at[0:levels], mats.at[stack : stack + levels]
        for j in range(0, size, 2):
            here = slice(j * width, (j + 2) * width)
            result = dot(top[...], lows[:, here]) + dot(rest[...], highs[:, here]) + dot(top[...], highs[:, here])
            put(j, result[:, :width])
            put(j + 1, result[:, width:])

    def back(i):
        return (2 * width - turn(i)) % width

    def from_left(block, rim, i, lv):
        return pltpu.roll(jnp.where(lane[lv] == width - 1, pltpu.roll(rim, back(i), 1), block), 1, 1)

    def from_right(block, rim, i, lv):
        return pltpu.roll(jnp.where(lane[lv] == 0, pltpu.roll(rim, back(i), 1), block), width - 1, 1)

    def forward_rows(n, which, lv):
        state, s = chain[0][n], spread[lv]
        keep = 1.0 - 4.0 * s
        values = []
        for i in which:
            v, before, after = state[i + 1, lv], state[i, lv], state[i + 2, lv]
            b = by[i, lv]
            left = from_left((b + s) * v, (pb[0, 0, lv] + s) * pv[n, 0, lv], i, lv)
            right = from_right(v, pv[n, 1, lv], i, lv)
            flow = (keep - ax[i + 1, lv] - b) * v + ax[i, lv] * before + left
            values.append(flow + s * (before + after + right))
        return values

    def adjoint_rows(n, which, lv):
        state, s = chain[1][n], spread[lv]
        keep = 1.0 - 4.0 * s
        values = []
        for i in which:
            w, before, after = state[i + 1, lv], state[i, lv], state[i + 2, lv]
            left = from_left(w, pw[n, 0, lv], i, lv)
            right = from_right(w, pw[n, 1, lv], i, lv)
            a, b = ax[i + 1, lv], by[i, lv]
            flow = (keep - a - b) * w + a * after + b * right
            values.append(flow + s * (before + after + left + right))
        return values

    def rim_parts(block):
        return (
            pltpu.roll(block, GROUP, 1), pltpu.roll(block, width - GROUP, 1),
            pltpu.roll(block, 1, 1), pltpu.roll(block, width - 1, 1),
        )

    def forward_rim(block, side, lv):
        before, after, left, right = rim_parts(block)
        s, a, b = spread[lv], pa[0, side, lv], pb[0, side, lv]
        flow = (1.0 - 4.0 * s - a - b) * block
        flow = flow + pltpu.roll(a, GROUP, 1) * before + pltpu.roll(b, 1, 1) * left
        return jnp.where(inside[side][lv], flow + s * (before + after + left + right), 0.0)

    def adjoint_rim(block, side, lv):
        before, after, left, right = rim_parts(block)
        s, a, b = spread[lv], pa[0, side, lv], pb[0, side, lv]
        flow = (1.0 - 4.0 * s - a - b) * block + a * after + b * right
        return jnp.where(inside[side][lv], flow + s * (before + after + left + right), 0.0)

    def put_all(state, shift, which, rims=None, n=0):
        def put(j, value):
            if j < len(which):
                state[which[j] + shift] = value
            else:
                rims[n, j - len(which)] = value

        return put

    def advance_rim(ref, n, rule, mats):
        mixed(mats, lambda lv: [rule(ref[n, side, lv], side, lv) for side in (0, 1)], 2, put_all(None, 0, [], ref, n + 1))

    def forward(n, steps, rim):
        which = mirror(*steps)
        target = (end, 0) if n == STEPS - 1 else (chain[0][n + 1], 1)

        def rule(lv):
            return forward_rows(n, which, lv) + [forward_rim(pv[n, side, lv], side, lv) for side in (0, 1) if rim]

        mixed(mat, rule, len(which) + 2 * rim, put_all(*target, which, pv, n + 1))

    def adjoint(n, steps, rim):
        which = mirror(*steps)
        if n == STEPS - 1:
            def body(t):
                pair = mirror(steps[0] - t)
                finish(out_incr, pair, lambda lv: [
                    gradient_v[i, lv] + value for i, value in zip(pair, adjoint_rows(n, pair, lv))
                ])

            loop(len(steps), body)
        else:
            def rule(lv):
                return adjoint_rows(n, which, lv) + [adjoint_rim(pw[n, side, lv], side, lv) for side in (0, 1) if rim]

            mixed(mat_t, rule, len(which) + 2 * rim, put_all(chain[1][n + 1], 1, which, pw, n + 1))

    def rim_entry(lv):
        own, far = q_dual[0, lv], outside[lv]
        both = []
        for side, (left, right) in enumerate(((far, own), (own, far))):
            value = jnp.where(near[lv], left, right)
            low = pltpu.roll(x_msg_up[1, lv], (-2 * GROUP * side) % width, 1)
            high = pltpu.roll(x_msg_down[1, lv], (GROUP * (rows + 2) - 2 * GROUP * side) % width, 1)
            value = jnp.where(place[lv] < 0, low, jnp.where(place[lv] >= rows, high, value))
            both.append(jnp.where(inside[side][lv], value, 0.0))
        return both

    def enter(lot):
        which = mirror(*inward[lot])
        arrived(u_recv, lot, len(which))
        pack_into(q_dual, 0, which, lambda i, lv: inbox[i, lv])
        if lot == 1:
            heard_both(m_up(1), m_down(1), x_first, x_last)
        rim = lot > 0

        def rule(lv):
            return [inbox[i, lv] for i in which] + (rim_entry(lv) if rim else [])

        mixed(mat_t, rule, len(which) + 2 * rim, put_all(w0, 1, which, pw, 0))

    done = [0] * STEPS

    def produce(n, steps):
        if n:
            while done[n - 1] < min(steps[-1] + 2, reach):
                first = done[n - 1]
                produce(n - 1, range(first, min(first + 2, reach)))
        edge = steps[-1] == reach - 1
        if edge:
            if n == 0:
                write_message(0, [ref[0, side] for ref in (pv, pb, pa) for side in (0, 1)])
                pl.when(not_(x_first))(lambda: a_up().wait_recv())
            if n == 1:
                read_message(0, [(ref, 0, side) for ref in (pv, pb, pa) for side in (0, 1)])
            with jax.named_scope(f'xheard0 {n}'): x_heard(0, n)
        if n == 1 and edge:
            advance_rim(pv, 0, forward_rim, mat)
        first = done[n]
        done[n] += len(steps)
        rim = (n == 0 and first < 3 <= done[n]) or (n == 1 and (first == 0 or edge))
        with jax.named_scope(f'fwd n={n} {list(steps)}'): forward(n, steps, False)
        if rim:
            advance_rim(pv, n, forward_rim, mat)
        if edge and n < STEPS - 1:
            x_start(0, n + 1)

    def produce_end(lot):
        produce(STEPS - 1, outward[lot])
        for i in mirror(*outward[lot]):
            end_copy(i, lot).start()

    def finish(out, which, values):
        sums = {}
        for lv in spans:
            size = lv.stop - lv.start
            for i, value in zip(which, values(lv)):
                out[pl.ds(lv.start * rows + i, size, stride=rows), :] = value
                sums[size] = sums[size] + value * value if size in sums else value * value
        for size, value in sums.items():
            acc[0:size] += value

    def finish_dual(lot, earlier):
        if earlier:
            arrived(e_recv, lot, 2 * len(outward[lot]))

        def body(t):
            pair = mirror(outward[lot][0] + t)
            finish(out_dual, pair, lambda lv: [
                forcing_v[i, lv] + end_in[i, lv] if earlier else forcing_v[i, lv] for i in pair
            ])

        loop(len(outward[lot]), body)

    def early_residuals(i):
        d, v = dual_v[i], v0[i + 1]
        forcing_v[i] = forcing_v[i] - error_v[i] * d - v
        gradient_v[i] = gradient_v[i] - obs_v[i] * v - d

    @pl.when(has_prev)
    def _():
        send_duals([0])
        loaded(3)
        pack_into(q_own, 3, range(rows), lambda i, lv: dual_v[i, lv])
        start_both(q_up(3), q_down(3), y_first, y_last)
        heard_both(q_up(3), q_down(3), y_first, y_last)
        out_send[...] = jnp.where(near, q_left[3], q_right[3])
        outside_copy().start()
        send_duals(range(1, len(inward)))

    @pl.when(has_next)
    def _():
        x_start(0, 0)
        pl.when(not_(x_last))(lambda: a_up().start())
        for n, (f, value) in enumerate(
            ((0, lambda i, lv: v0[i + 1, lv]), (1, lambda i, lv: by[i, lv]), (2, lambda i, lv: ax[i + 1, lv]))
        ):
            loaded(f)
            pack_into(q_own, n, range(rows), value)
            with jax.named_scope(f'qsent {n}'): start_both(q_up(n), q_down(n), y_first, y_last)

    pl.when(not_(has_next))(lambda: loaded(0, 1, 2))
    for line, semaphore in ((lines[1], met.at[0]),):
        greet(semaphore, line)

    @pl.when(has_next)
    def _():
        for n, ref in enumerate((pv, pb, pa)):
            with jax.named_scope(f'qheard {n}'): heard_both(q_up(n), q_down(n), y_first, y_last)
            assemble(ref, 0, q_own[n], q_left[n], q_right[n])
        for lot in range(len(outward) - 2):
            produce_end(lot)

    for f in range(3, FIELDS):
        if f == 3:
            pl.when(not_(has_prev))(lambda: loaded(3))
        else:
            loaded(f)
    with jax.named_scope('early'): loop(rows, early_residuals)

    @pl.when(not_(has_prev))
    def _():
        for lot in range(len(outward)):
            finish_dual(lot, False)

    with jax.named_scope('met0'): pl.semaphore_wait(met.at[0], nx - 1)
    greet(met.at[1], lines[0])

    @pl.when(has_next)
    def _():
        with jax.named_scope('enter0'): enter(0)
        x_start(1, 0)
        produce_end(len(outward) - 2)
        with jax.named_scope('O'): outside_copy().wait_recv()
        own, far = q_dual[0], outside[...]
        assemble(pu, 0, own, far, far)
        write_message(1, [pu[0, 0], pu[0, 1]])
        floor = [reach] * STEPS
        for lot in range(1, len(inward)):
            with jax.named_scope(f'enter {lot}'): enter(lot)
            least = inward[lot][-1]
            for n in range(min(lot, STEPS) if least else STEPS):
                low = least + 1 + n if least else 0
                lots = paired(range(floor[n] - 1, low - 1, -1))
                for t, steps in enumerate(lots):
                    edge = steps[0] == reach - 1
                    if edge:
                        with jax.named_scope(f'xheard1 {n}'): x_heard(1, n)
                    with jax.named_scope(f'adj n={n} {list(steps)}'): adjoint(n, steps, t == len(lots) - 1)
                    if edge and n < STEPS - 1:
                        x_start(1, n + 1)
                floor[n] = min(floor[n], low)
            if lot == 1:
                produce_end(len(outward) - 1)

    @pl.when(not_(has_next))
    def _():
        for lot in range(len(outward)):
            def body(t):
                pair = mirror(outward[lot][0] + t)
                finish(out_incr, pair, lambda lv: [gradient_v[i, lv] for i in pair])

            loop(len(outward[lot]), body)

    @pl.when(has_prev)
    def _():
        for lot in range(len(outward)):
            with jax.named_scope(f'fd {lot}'): finish_dual(lot, True)

    pl.semaphore_wait(met.at[1], windows - 1)
    part[...] = jnp.sum(acc[...], axis=0, keepdims=True)
    parts[me] = part[...]

    def coords(flat):
        return {"tm": flat // (nx * ny), "gx": (flat // ny) % nx, "gy": flat % ny}

    def tell(d):
        other = (me + d) % count
        return remote(part, parts.at[me], r_send, r_recv, coords(other))

    with jax.named_scope('tell'): loop(count, lambda d: tell(d).start(), 1)

    pl.when(has_prev)(lambda: left_all(u_send))

    @pl.when(has_prev)
    def _():
        outside_copy().wait_send()
        sent_both(q_up(3), q_down(3), y_first, y_last)

    @pl.when(has_next)
    def _():
        left_all(e_send)
        pl.when(not_(x_last))(lambda: a_up().wait_send())
        for n in range(STEPS):
            sent_both(x_up(0, n), x_down(0, n), x_first, x_last)
            sent_both(x_up(1, n), x_down(1, n), x_first, x_last)
            sent_both(q_up(n), q_down(n), y_first, y_last)
        for n in range(2):
            sent_both(m_up(n), m_down(n), x_first, x_last)

    others = parts.at[pl.ds(0, count - 1)]
    every = remote(others, others, r_send, r_recv, {"tm": k})
    with jax.named_scope('hear'): every.wait_recv()
    total = jnp.sum(jnp.sum(parts[...], axis=0), axis=1, keepdims=True)
    cells = 2 * rows * levels * width * count
    root_mean = jnp.sqrt(total / cells + 1e-06)
    out_scale[...] = jnp.broadcast_to(jnp.minimum(1.0, 0.5 / root_mean), out_scale.shape)
    every.wait_send()


def update(scale, dual, increment, residual_dual, residual_incr, dual_next, incr_next, dual_v, incr_v, sem):
    size = dual.shape[0]
    chunk = -(-size // (4 * 8)) * 8
    copies = []
    for lot, start in enumerate(range(0, size, chunk)):
        span = pl.ds(start, min(chunk, size - start))
        for j, (now, rest, home, out) in enumerate((
            (dual, residual_dual, dual_v, dual_next), (increment, residual_incr, incr_v, incr_next)
        )):
            for low in range(start, min(start + chunk, size), 64):
                piece = pl.ds(low, min(64, start + chunk - low, size - low))
                home[piece, :] = now[piece, :] + scale[...] * rest[piece, :]
            copies.append(pltpu.make_async_copy(home.at[span], out.at[span], sem.at[j, lot]))
            copies[-1].start()
    for copy in copies:
        copy.wait()


def local(axes, increment, dual_state, forcing, gradient, courant_x, courant_y, error_var, obs_weight, diffusion, level_mix):
    levels, rows, width = increment.shape[1:]
    count = axes[0] * axes[1] * axes[2]
    stack = -(-levels // 16) * 16
    reach = rows // 2
    assert rows % 4 == 0 and rows >= 8 and GROUP * (rows + 4) <= width
    fields = [
        part.reshape(levels, rows, 1, width)
        for part in (increment, dual_state, forcing, gradient, courant_x, courant_y, error_var, obs_weight)
    ]
    fields = [pltpu.with_memory_space_constraint(part, pltpu.HBM) for part in fields]
    slab = lambda *lead: pltpu.VMEM((*lead, levels, width), jnp.float32)
    dma = lambda *shape: pltpu.SemaphoreType.DMA(shape)
    one = pltpu.SemaphoreType.DMA
    scratch = [
        *[slab(rows + 2)] * 6, slab(rows + 1), slab(rows), slab(rows), slab(rows), slab(rows),
        slab(4), slab(4), slab(4), slab(), slab(1), slab(), slab(2, 2), slab(2), slab(2),
        slab(3, 2), slab(1, 2), slab(3, 2), slab(1, 2), slab(1, 2),
        slab(rows), slab(rows), slab(rows), slab(rows), slab(rows),
        slab(), pltpu.VMEM((levels, levels), jnp.float32), pltpu.VMEM((1, levels), jnp.float32),
        pltpu.VMEM((2 * stack, levels), jnp.bfloat16), pltpu.VMEM((2 * stack, levels), jnp.bfloat16),
        *[pltpu.VMEM((2, levels, 8 * width), jnp.bfloat16)] * 2,
        pltpu.VMEM((16, width), jnp.float32), pltpu.VMEM((1, width), jnp.float32), pltpu.VMEM((count, 1, width), jnp.float32),
        dma(FIELDS), dma(2), one, dma(reach), one, dma(reach), dma(2),
        dma(2, STEPS, 2), dma(2, STEPS, 2), one, one, dma(4, 2), dma(4, 2), dma(2, 2), dma(2, 2),
        one, one, pltpu.SemaphoreType.REGULAR((2,)),
    ]
    field = jax.ShapeDtypeStruct((levels * rows, width), jnp.float32)
    vmem = pl.BlockSpec(memory_space=pltpu.VMEM)
    anywhere = pl.BlockSpec(memory_space=pltpu.HBM)
    residual_dual, residual_incr, scale = pl.pallas_call(
        functools.partial(kernel, axes),
        out_shape=(field, field, jax.ShapeDtypeStruct((1, width), jnp.float32)),
        in_specs=[anywhere] * 10,
        out_specs=(vmem, vmem, vmem),
        scratch_shapes=scratch,
        compiler_params=pltpu.CompilerParams(
            collective_id=0, has_side_effects=True, vmem_limit_bytes=32 * 1024 * 1024
        ),
    )(*fields, *(pltpu.with_memory_space_constraint(part, pltpu.HBM) for part in (diffusion[None, :], level_mix)))
    flat = lambda part: part.reshape(levels * rows, width)
    results = pl.pallas_call(
        update,
        out_shape=(field, field),
        in_specs=[vmem] * 5,
        out_specs=(anywhere, anywhere),
        scratch_shapes=[pltpu.VMEM(field.shape, jnp.float32)] * 2 + [dma(2, 4)],
        compiler_params=pltpu.CompilerParams(vmem_limit_bytes=16 * 1024 * 1024),
    )(scale, flat(dual_state), flat(increment), residual_dual, residual_incr)
    return tuple(part.reshape(increment.shape) for part in results)


def solution(mesh):
    spec = P("tm", None, "gx", "gy")
    axes = tuple(mesh.shape[name] for name in ("tm", "gx", "gy"))
    return jax.shard_map(
        functools.partial(local, axes),
        mesh=mesh,
        in_specs=(spec,) * FIELDS + (P(), P()),
        out_specs=(spec, spec),
        check_vma=False,
    )
```
